128 devices in a mesh: dp: 64 (over z, y, x), fsdp: 2 (over core).
Axes of the slice: x: 4, y: 4, z: 4, core: 2. Of those that a mesh axis runs over, the one named last changes fastest.
Arguments:
- patches: bfloat16 [4096, 32, 1024], P(('dp', 'fsdp')), may hold values from -6 to 6
- rows: int32 [4096, 32], P(('dp', 'fsdp')), may hold values from 0 to 63
- cols: int32 [4096, 32], P(('dp', 'fsdp')), may hold values from 0 to 63
- keep: int32 [4096, 32], P(('dp', 'fsdp')), may hold values from 0 to 1, as said below
- images: int32 [4096, 32], P(('dp', 'fsdp')), may hold values from 0 to 3, never falling along the last dimension, each value on 1 to 16 neighbouring positions
- destination: int32 [2, 64, 32], P('fsdp'), may hold values from 0 to 63, as said below
- row_table: bfloat16 [64, 1024], replicated, may hold values from -6 to 6
- col_table: bfloat16 [64, 1024], replicated, may hold values from -6 to 6
- w_qkv: bfloat16 [1024, 3072], P('fsdp'), may hold values from -1 to 1
- w_out: bfloat16 [1024, 1024], P('fsdp'), may hold values from -0.1875 to 0.1875
- w_up: bfloat16 [1024, 4096], P('fsdp'), may hold values from -0.1875 to 0.1875
- w_down: bfloat16 [4096, 1024], P('fsdp'), may hold values from -0.09375 to 0.09375
Outputs:
- encoded: bfloat16 [4096, 32, 1024], P(('dp', 'fsdp'))
The draws below stay inside these ranges and needn't reach their ends.
Inputs may be any that keep to these rules, and one draw needn't show every extreme that they name: keep is 0 or 1; the share of kept tokens differs from sequence to sequence. `destination`: for each fsdp index, every dp index is named by exactly 32 entries of the table, and no row names one dp index more than 1 times.
All inputs are finite; a program needn't handle non-finite values.
Results may differ from the reference program's by a relative error of at most 0.0065.
Values may be sent and summed in bfloat16 or wider, within the bound.
No kernel may reach another device: no remote copies, remote signals or barrier semaphores. Data moves between devices by JAX's collectives and lax.ppermute only.
A program may use at most 192 MiB of HBM per device.

```python
import math
import jax
import jax.numpy as jnp
import numpy as np
from jax import lax

D = 1024
HEADS = 16
HEAD_DIM = 64
MLP = 4096
SEQ = 32
IMGS = 4
GRID = 64
BLK = 32
PEERS = 64
CAP = 1
BLOCKS = 4096
N_FSDP = 2


def draw_keep(key, part):
    rate_key, coin_key = jax.random.split(jax.random.fold_in(key, 11))
    rates = jax.random.randint(rate_key, (BLOCKS, 1), 30, 96)
    coins = jax.random.randint(coin_key, (BLOCKS, SEQ), 0, 100)
    return (coins < rates).astype(jnp.int32)


def draw_destination(key, part):

    def one_group(group_key):
        first, second, third, fourth = jax.random.split(group_key, 4)
        row_perm = jax.random.permutation(first, PEERS)
        offsets = jnp.tile(jax.random.permutation(second, PEERS), CAP)[:BLK]
        symbol = jax.random.permutation(third, PEERS)
        shuffle = jax.vmap(lambda inner: jax.random.permutation(inner, BLK))(jax.random.split(fourth, PEERS))
        chosen = offsets[shuffle]
        return symbol[(row_perm[:, None] + chosen) % PEERS].astype(jnp.int32)
    return jax.vmap(one_group)(jax.random.split(jax.random.fold_in(key, 23), N_FSDP))


def draw_w_qkv(key, part):
    base_key = jax.random.fold_in(jax.random.fold_in(key, 37), 0)
    base = jnp.clip(jax.random.normal(base_key, (D, 3 * D), jnp.float32), -6.0, 6.0) * D ** (-0.5)
    return jnp.clip(base, -1.0, 1.0).astype(jnp.bfloat16)


def set_ends(entries, own_key, low, high):
    spot = [jax.random.randint(jax.random.fold_in(own_key, axis), (), 0, length) for axis, length in enumerate(entries.shape)]
    main_axis = entries.shape.index(max(entries.shape))
    beside = spot[:main_axis] + [(spot[main_axis] + 1) % entries.shape[main_axis]] + spot[main_axis + 1:]
    return entries.at[tuple(spot)].set(low).at[tuple(beside)].set(high)


def shard_levels(rng, extent, pieces, least, high):
    gain, own = 1.0, jax.random.fold_in(rng, 6)
    for axis_at, blocks in pieces:
        draws = jnp.exp(jax.random.uniform(jax.random.fold_in(own, axis_at), (blocks,), jnp.float32, least / len(pieces), high / len(pieces)))
        gain = gain * jnp.repeat(draws, extent[axis_at] // blocks).reshape([-1 if axis == axis_at else 1 for axis in range(len(extent))])
    return gain


def profile(number_of, total, bound, skew):
    portions = [(1 << 20) // math.isqrt(grade ** skew) + 1 for grade in range(2, number_of + 1)]
    rest, counts = total - bound - (number_of - 1), [1] * (number_of - 1)
    while rest > 0:
        candidates = [i for i in range(number_of - 1) if counts[i] < bound]
        mass, remaining = sum([portions[i] for i in candidates]), rest
        for i in candidates:
            more = min(bound - counts[i], max(1, remaining * portions[i] // mass), rest)
            counts[i] = counts[i] + more
            rest = rest - more
    return np.array([bound] + counts)


def ragged(own_key, number_of, total, bound, lean):
    if number_of == 2:
        one = jax.random.randint(own_key, (), max(1, total - bound), min(bound, total - 1) + 1)
        return jnp.stack([one, total - one])
    sizes = jnp.asarray(profile(number_of, total, bound, lean), jnp.int32)
    couples = (number_of - 1) // 2
    donor, sink = sizes[1:1 + 2 * couples:2], sizes[2:2 + 2 * couples:2]
    room = jnp.minimum(donor - 1, bound - sink)
    moved = jax.random.randint(jax.random.fold_in(own_key, 1), (couples,), 0, 1 << 20) % (room + 1)
    sizes = sizes.at[1:1 + 2 * couples:2].set(donor - moved).at[2:2 + 2 * couples:2].set(sink + moved)
    return sizes[jax.random.permutation(jax.random.fold_in(own_key, 2), number_of)]


def bell_draw(stream_key, dims, scale, most, pieces=(), kind=jnp.bfloat16):
    drawn = jax.random.normal(stream_key, dims, jnp.float32) * scale
    if len(pieces) > 0:
        drawn = shard_levels(stream_key, dims, pieces, -0.22, 0.18) * drawn
    return jnp.clip(drawn, min=-most, max=most).astype(kind)


def setup_inputs(seed: int = 0) -> dict:
    splits = jax.random.split(jax.random.key(seed), 13)
    patches = bell_draw(splits[0], (BLOCKS, SEQ, D), 1.0, 6.0, ((0, 128),))
    rows = set_ends(jax.random.randint(splits[1], (BLOCKS, SEQ), 0, GRID), jax.random.fold_in(splits[1], 1), 0, GRID - 1).astype(jnp.int32)
    cols = set_ends(jax.random.randint(splits[2], (BLOCKS, SEQ), 0, GRID), jax.random.fold_in(splits[2], 1), 0, GRID - 1).astype(jnp.int32)
    keep = draw_keep(jax.random.fold_in(splits[12], 71), 0)
    images = jax.vmap(lambda own: jnp.searchsorted(jnp.cumsum(ragged(own, IMGS, SEQ, SEQ // 2, 0)), jnp.arange(SEQ), side="right"))(jax.random.split(splits[4], BLOCKS)).reshape((BLOCKS, SEQ)).astype(jnp.int32)
    destination = draw_destination(jax.random.fold_in(splits[12], 71), 0)
    row_table = bell_draw(splits[6], (GRID, D), 1.0, 6.0)
    col_table = bell_draw(splits[7], (GRID, D), 1.0, 6.0)
    w_qkv = draw_w_qkv(jax.random.fold_in(splits[12], 71), 0)
    w_out = bell_draw(splits[9], (D, D), D ** -0.5, 0.1875, ((0, 2),))
    w_up = bell_draw(splits[10], (D, MLP), D ** -0.5, 0.1875, ((0, 2),))
    w_down = bell_draw(splits[11], (MLP, D), MLP ** -0.5, 0.09375, ((0, 2),))
    return {"patches": patches, "rows": rows, "cols": cols, "keep": keep, "images": images, "destination": destination, "row_table": row_table, "col_table": col_table, "w_qkv": w_qkv, "w_out": w_out, "w_up": w_up, "w_down": w_down}


EPS = 1e-06

def layer_norm(values):
    center = values - lax.optimization_barrier(jnp.mean(values, axis=-1, keepdims=True))
    spread = lax.optimization_barrier(jnp.mean(center * center, axis=-1, keepdims=True))
    return center * lax.rsqrt(spread + EPS)

def embed(patches, rows, cols, row_table, col_table):
    slots = jnp.arange(GRID, dtype=jnp.int32)
    onehot = jnp.concatenate([(rows[..., None] == slots).astype(jnp.float32), (cols[..., None] == slots).astype(jnp.float32)], axis=-1)
    tables = jnp.concatenate([row_table, col_table], axis=0).astype(jnp.float32)
    places = jnp.einsum('nsg,gd->nsd', onehot, tables)
    return (patches.astype(jnp.float32) + places).astype(jnp.bfloat16)

def encode(embedded, label, w_qkv, w_out, w_up, w_down):
    count, seq, width = embedded.shape
    inputs = embedded.astype(jnp.float32).reshape(count * seq, width)
    normed = layer_norm(inputs).astype(jnp.bfloat16)
    qkv = jnp.dot(normed, w_qkv, preferred_element_type=jnp.float32).astype(jnp.bfloat16)
    parts = qkv.reshape(count, seq, 3, HEADS, HEAD_DIM).astype(jnp.float32)
    scores = jnp.einsum('nqhd,nkhd->nhqk', parts[:, :, 0], parts[:, :, 1]) * HEAD_DIM ** (-0.5)
    allowed = (label[:, :, None] == label[:, None, :]) & (label[:, None, :] > 0)
    allowed = allowed[:, None]
    scores = jnp.where(allowed, scores, -1e+30)
    peak = lax.optimization_barrier(jnp.max(scores, axis=-1, keepdims=True))
    weights = jnp.where(allowed, jnp.exp(scores - peak), 0.0)
    dropped = (label == 0).astype(jnp.float32)[:, None, :, None]
    total = lax.optimization_barrier(jnp.sum(weights, axis=-1, keepdims=True)) + dropped
    probs = (weights / total).astype(jnp.bfloat16).astype(jnp.float32)
    attended = jnp.einsum('nhqk,nkhd->nqhd', probs, parts[:, :, 2]).astype(jnp.bfloat16)
    mid = inputs + jnp.dot(attended.reshape(count * seq, width), w_out, preferred_element_type=jnp.float32)
    second = layer_norm(mid).astype(jnp.bfloat16)
    upper = jnp.dot(second, w_up, preferred_element_type=jnp.float32)
    activated = jax.nn.gelu(upper, approximate=True).astype(jnp.bfloat16)
    result = mid + jnp.dot(activated, w_down, preferred_element_type=jnp.float32)
    live = label.reshape(count * seq, 1) > 0
    return jnp.where(live, result, 0.0).astype(jnp.bfloat16).reshape(count, seq, width)

def placement_order(destination):
    groups, peers, blk = destination.shape
    targets = jnp.arange(peers, dtype=jnp.int32)
    hits = (destination[..., None] == targets).astype(jnp.int32)
    per_source = lax.optimization_barrier(jnp.sum(hits, axis=2)).astype(jnp.int32)
    before = (jnp.cumsum(per_source, axis=1) - per_source).astype(jnp.int32)
    base = jnp.take_along_axis(before, destination, axis=2).astype(jnp.int32)
    within = (jnp.cumsum(hits, axis=2) - hits).astype(jnp.int32)
    within_at = lax.optimization_barrier(jnp.sum(within * hits, axis=3)).astype(jnp.int32)
    rank_at = base + within_at
    group_ids = jnp.arange(groups, dtype=jnp.int32)[:, None, None]
    source_ids = jnp.arange(peers, dtype=jnp.int32)[None, :, None]
    block_ids = jnp.arange(blk, dtype=jnp.int32)[None, None, :]
    source = (source_ids * groups + group_ids) * blk + block_ids
    target = (destination * groups + group_ids) * blk + rank_at
    order = jnp.zeros((groups * peers * blk,), jnp.int32)
    return order.at[target.reshape(-1).astype(jnp.int32)].set(source.reshape(-1).astype(jnp.int32))

def reference(patches, rows, cols, keep, images, destination, row_table, col_table, w_qkv, w_out, w_up, w_down):
    embedded = embed(patches, rows, cols, row_table, col_table)
    label = keep * (images + 1)
    total_blocks = embedded.shape[0]
    grouped = embedded.reshape(total_blocks // BLK, BLK, SEQ, D)
    labels = label.reshape(total_blocks // BLK, BLK, SEQ)

    def one_group(pair):
        return encode(pair[0], pair[1], w_qkv, w_out, w_up, w_down)
    processed = lax.map(one_group, (grouped, labels)).reshape(total_blocks, SEQ, D)
    order = placement_order(destination)
    return jnp.take(processed, order, axis=0)
```

```python
import jax
import jax.numpy as jnp
from jax import lax
from jax.experimental import pallas as pl
from jax.experimental.pallas import tpu as pltpu
from jax.sharding import PartitionSpec as P

HEADS = 16
HEAD_DIM = 64
BLK = 32
SEQ = 32
D = 1024
MLP = 4096
PEERS = 64
ROWS = BLK * SEQ
COLS = D // 128
SLOT = COLS * SEQ + 8
GROUP = 4
EPS = 1e-06
MASKED = -1e30
ANY = pl.BlockSpec(memory_space=pl.ANY)
SMEM = pl.BlockSpec(memory_space=pltpu.SMEM)
VMEM = pl.BlockSpec(memory_space=pltpu.VMEM)


def norm(values):
    center = values - jnp.mean(values, axis=-1, keepdims=True)
    spread = jnp.mean(center * center, axis=-1, keepdims=True)
    return center * lax.rsqrt(spread + EPS)


def gelu(x):
    inner = x * (0.7978845608028654 + 0.035677408136300125 * (x * x))
    half = 0.5 * x
    return half + half * jnp.tanh(inner)


def embed_body(slots, onehot, tables, patches, marks, out, buf, sem):
    def group(g, carry):
        first = g * GROUP
        places = jnp.dot(
            onehot[pl.ds(g * 128, 128), :], tables[...], preferred_element_type=jnp.float32
        )
        for j in range(GROUP):
            k = first + j
            block = patches[k].astype(jnp.float32) + places[j * SEQ:(j + 1) * SEQ, :]
            block = block.astype(jnp.bfloat16)
            for c in range(COLS):
                buf[k, c * SEQ:(c + 1) * SEQ, :] = block[:, c * 128:(c + 1) * 128]
            buf[k, COLS * SEQ:, :] = marks[k]
            pltpu.make_async_copy(buf.at[k], out.at[slots[k]], sem.at[k]).start()
        return carry

    lax.fori_loop(0, BLK // GROUP, group, 0)
    for k in range(BLK):
        pltpu.make_async_copy(buf.at[k], out.at[slots[k]], sem.at[k]).wait()


def embed_slots(slots, onehot, tables, patches, marks):
    return pl.pallas_call(
        embed_body,
        out_shape=jax.ShapeDtypeStruct((PEERS, SLOT, 128), jnp.bfloat16),
        in_specs=[SMEM, VMEM, VMEM, VMEM, VMEM],
        out_specs=ANY,
        scratch_shapes=[
            pltpu.VMEM((BLK, SLOT, 128), jnp.bfloat16),
            pltpu.SemaphoreType.DMA((BLK,)),
        ],
        compiler_params=pltpu.CompilerParams(vmem_limit_bytes=32 * 1024 * 1024),
        name="embed",
    )(slots, onehot, tables, patches, marks)


def sequence(xs, k):
    return jnp.concatenate([xs[k, c * SEQ:(c + 1) * SEQ, :] for c in range(COLS)], axis=1)


def layer_body(
    side, order, arrived, q0, q1, o0, o1, u0, u1, d0, d1, out,
    xs, w_qkv, w_out, w_up, w_down, normed, qkv, mid, act, outb, live, in_sem, w_sem, out_sem,
):
    mine = side[0]
    pairs = [(q0, q1, w_qkv, D), (o0, o1, w_out, D), (u0, u1, w_up, D), (d0, d1, w_down, MLP)]

    def weight_copies(i):
        own, other, whole, rows = pairs[i]
        half = rows // 2
        return (
            pltpu.make_async_copy(own, whole.at[pl.ds(mine * half, half), :], w_sem.at[2 * i]),
            pltpu.make_async_copy(
                other, whole.at[pl.ds((1 - mine) * half, half), :], w_sem.at[2 * i + 1]
            ),
        )

    def in_copy(k):
        return pltpu.make_async_copy(arrived.at[order[k]], xs.at[k], in_sem.at[k])

    def out_copy(k):
        return pltpu.make_async_copy(outb.at[k], out.at[k], out_sem.at[k])

    for k in range(BLK):
        in_copy(k).start()
    for i in range(4):
        for copy in weight_copies(i):
            copy.start()
    for k in range(BLK):
        in_copy(k).wait()

    def first_norm(g, carry):
        for j in range(GROUP):
            k = g * GROUP + j
            x = sequence(xs, k).astype(jnp.float32)
            normed[pl.ds(k * SEQ, SEQ), :] = norm(x).astype(jnp.bfloat16)
        return carry

    lax.fori_loop(0, BLK // GROUP, first_norm, 0)
    for copy in weight_copies(0):
        copy.wait()

    def project(n, carry):
        for m in range(2):
            part = jnp.dot(
                normed[m * 512:(m + 1) * 512, :], w_qkv[:, pl.ds(n * 512, 512)],
                preferred_element_type=jnp.float32,
            )
            qkv[m * 512:(m + 1) * 512, pl.ds(n * 512, 512)] = part.astype(jnp.bfloat16)
        return carry

    lax.fori_loop(0, 6, project, 0)
    lane = lax.broadcasted_iota(jnp.int32, (128, 128), 1)
    line = lax.broadcasted_iota(jnp.int32, (128, 128), 0)
    low = lane < HEAD_DIM
    zero = jnp.zeros((128, 128), jnp.bfloat16)
    one = jnp.ones((128, 128), jnp.bfloat16)
    ones = jnp.concatenate([jnp.where(low, one, zero), jnp.where(low, zero, one)], axis=0)

    def attend(g, carry):
        base = pl.multiple_of(g * 128, 128)
        label = jnp.zeros((8, 128), jnp.float32)
        for j in range(GROUP):
            marks = xs[g * GROUP + j, COLS * SEQ:, :].astype(jnp.float32)
            label = jnp.where(lane[:8] // SEQ == j, marks, label)
        wide = jnp.broadcast_to(label[:1], (128, 128))
        column = jnp.sum(jnp.where(lane == line, wide, 0.0), axis=1, keepdims=True)
        live[pl.ds(base, 128), :] = jnp.broadcast_to(column, (128, 128))
        allowed = (column == wide) & (wide > 0.0) & (lane // SEQ == line // SEQ)
        bias = jnp.where(allowed, 0.0, MASKED)
        bias = jnp.concatenate([bias, bias], axis=0)
        dropped = jnp.where(column == 0.0, 1.0, 0.0)
        for h in range(HEADS // 2):
            q = qkv[pl.ds(base, 128), h * 128:(h + 1) * 128] * jnp.bfloat16(HEAD_DIM ** -0.5)
            key = qkv[pl.ds(base, 128), D + h * 128:D + (h + 1) * 128]
            value = qkv[pl.ds(base, 128), 2 * D + h * 128:2 * D + (h + 1) * 128]
            both = jnp.concatenate([jnp.where(low, q, zero), jnp.where(low, zero, q)], axis=0)
            scores = lax.dot_general(
                both, key, (((1,), (1,)), ((), ())), preferred_element_type=jnp.float32
            )
            scores = scores + bias
            peak = jnp.maximum(jnp.max(scores, axis=1, keepdims=True), 0.1 * MASKED)
            weights = jnp.exp(scores - peak).astype(jnp.bfloat16)
            weights = jnp.concatenate([weights[:128], weights[128:]], axis=1)
            stacked = jnp.concatenate(
                [jnp.where(low, value, zero), jnp.where(low, zero, value)], axis=0
            )
            stacked = jnp.concatenate([stacked, ones], axis=1)
            mixed = jnp.dot(weights, stacked, preferred_element_type=jnp.float32)
            result = mixed[:, :128] / (mixed[:, 128:] + dropped)
            normed[pl.ds(base, 128), h * 128:(h + 1) * 128] = result.astype(jnp.bfloat16)
        return carry

    lax.fori_loop(0, BLK // GROUP, attend, 0)
    for copy in weight_copies(1):
        copy.wait()

    def merge(m, carry):
        base = pl.multiple_of(m * 256, 256)
        part = jnp.dot(
            normed[pl.ds(base, 256), :], w_out[...], preferred_element_type=jnp.float32
        )
        for j in range(8):
            k = m * 8 + j
            total = sequence(xs, k).astype(jnp.float32) + part[j * SEQ:(j + 1) * SEQ, :]
            mid[pl.ds(k * SEQ, SEQ), :] = total
            normed[pl.ds(k * SEQ, SEQ), :] = norm(total).astype(jnp.bfloat16)
        return carry

    lax.fori_loop(0, 4, merge, 0)
    for copy in weight_copies(2):
        copy.wait()

    def up(n, carry):
        for m in range(2):
            part = jnp.dot(
                normed[m * 512:(m + 1) * 512, :], w_up[:, pl.ds(n * 512, 512)],
                preferred_element_type=jnp.float32,
            )
            act[m * 512:(m + 1) * 512, pl.ds(n * 512, 512)] = gelu(part).astype(jnp.bfloat16)
        return carry

    lax.fori_loop(0, 8, up, 0)
    for copy in weight_copies(3):
        copy.wait()

    def down(m, carry):
        base = pl.multiple_of(m * 256, 256)
        part = jnp.dot(act[pl.ds(base, 256), :], w_down[...], preferred_element_type=jnp.float32)
        total = mid[pl.ds(base, 256), :] + part
        total = jnp.where(live[pl.ds(base, 256), :][:, :1] > 0.0, total, 0.0)
        total = total.astype(jnp.bfloat16)
        for j in range(8):
            k = m * 8 + j
            outb[k] = total[j * SEQ:(j + 1) * SEQ, :]
            out_copy(k).start()
        return carry

    lax.fori_loop(0, 4, down, 0)
    for k in range(BLK):
        out_copy(k).wait()


def layer(side, order, arrived, *weights):
    bf, f32 = jnp.bfloat16, jnp.float32
    return pl.pallas_call(
        layer_body,
        out_shape=jax.ShapeDtypeStruct((BLK, SEQ, D), bf),
        in_specs=[SMEM, SMEM] + [ANY] * 9,
        out_specs=ANY,
        scratch_shapes=[
            pltpu.VMEM((BLK, SLOT, 128), bf),
            pltpu.VMEM((D, 3 * D), bf),
            pltpu.VMEM((D, D), bf),
            pltpu.VMEM((D, MLP), bf),
            pltpu.VMEM((MLP, D), bf),
            pltpu.VMEM((ROWS, D), bf),
            pltpu.VMEM((ROWS, 3 * D), bf),
            pltpu.VMEM((ROWS, D), f32),
            pltpu.VMEM((ROWS, MLP), bf),
            pltpu.VMEM((BLK, SEQ, D), bf),
            pltpu.VMEM((ROWS, 128), f32),
            pltpu.SemaphoreType.DMA((BLK,)),
            pltpu.SemaphoreType.DMA((8,)),
            pltpu.SemaphoreType.DMA((BLK,)),
        ],
        compiler_params=pltpu.CompilerParams(vmem_limit_bytes=60 * 1024 * 1024),
        name="layer",
    )(side, order, arrived, *weights)


def arrivals(table, myself):
    filled = jnp.any(table == myself, axis=1)
    places = jnp.arange(PEERS, dtype=jnp.int32)
    rank = jnp.sum((filled[None, :] & (places[None, :] < places[:, None])).astype(jnp.int32), axis=1)
    wanted = jnp.arange(BLK, dtype=jnp.int32)
    hit = filled[None, :] & (rank[None, :] == wanted[:, None])
    return jnp.sum(jnp.where(hit, places[None, :], 0), axis=1)


def local(
    patches, rows, cols, keep, images, destination, row_table, col_table, w_qkv, w_out, w_up, w_down
):
    myself = lax.axis_index("dp")
    side = lax.axis_index("fsdp").astype(jnp.int32).reshape(1)
    swap = [(0, 1), (1, 0)]
    weights = []
    for w in (w_qkv, w_out, w_up, w_down):
        weights += [w, lax.ppermute(w, "fsdp", swap)]
    grid = row_table.shape[0]
    slots = jnp.arange(2 * grid, dtype=jnp.int32)
    spot = jnp.where(slots < grid, rows.reshape(-1, 1), cols.reshape(-1, 1) + grid)
    onehot = (spot == slots).astype(jnp.bfloat16)
    tables = jnp.concatenate([row_table, col_table], axis=0)
    labels = (keep * (images + 1)).astype(jnp.bfloat16)
    marks = jnp.broadcast_to(jnp.tile(labels, (1, GROUP))[:, None, :], (BLK, 8, 128))
    table = destination[0]
    mine = lax.dynamic_index_in_dim(table, myself, 0, keepdims=False)
    outgoing = embed_slots(mine, onehot, tables, patches, marks)
    arrived = lax.all_to_all(outgoing, "dp", split_axis=0, concat_axis=0, tiled=True)
    order = arrivals(table, myself)
    return layer(side, order, arrived, *weights)


def solution(mesh):
    whole = P(("dp", "fsdp"), None, None)
    flat = P(("dp", "fsdp"), None)
    half = P("fsdp", None)
    in_specs = (
        whole, flat, flat, flat, flat, P("fsdp", None, None), P(), P(), half, half, half, half,
    )
    return jax.shard_map(local, mesh=mesh, in_specs=in_specs, out_specs=whole, check_vma=False)
```

```python
import jax
import jax.numpy as jnp
from jax import lax
from jax.experimental import pallas as pl
from jax.experimental.pallas import tpu as pltpu
from jax.sharding import PartitionSpec as P


HEADS = 16
HEAD_DIM = 64
BLK = 32
SEQ = 32
D = 1024
MLP = 4096
PEERS = 64
GRID = 64
ROWS = BLK * SEQ
COLS = D // 128
SLOT = COLS * SEQ + 8
GROUP = 4
EPS = 1e-06
MASKED = -1e30
VMEM_LIMIT = 60 * 1024 * 1024
ANY = pl.BlockSpec(memory_space=pl.ANY)
HBM = pl.BlockSpec(memory_space=pltpu.HBM)
SMEM = pl.BlockSpec(memory_space=pltpu.SMEM)
VMEM = pl.BlockSpec(memory_space=pltpu.VMEM)


def norm(values):
    center = values - jnp.mean(values, axis=-1, keepdims=True)
    spread = jnp.mean(center * center, axis=-1, keepdims=True)
    return center * lax.rsqrt(spread + EPS)


def gelu(x):
    inner = x * (0.7978845608028654 + 0.035677408136300125 * (x * x))
    half = 0.5 * x
    return half + half * jnp.tanh(inner)


def embed_body(
    place, table, rows, cols, keep, images, row_table, col_table, patches, out,
    buf, raw, tables, marks, in_sem, sem,
):
    me, side = place[0], place[1]

    def in_copy(g):
        part = pl.ds(g * GROUP, GROUP)
        return pltpu.make_async_copy(patches.at[part], raw.at[part], in_sem.at[g])

    def out_copy(k):
        slot = jnp.where(side == 0, table[0, me, k], k)
        return pltpu.make_async_copy(buf.at[k], out.at[slot], sem.at[k])

    for g in range(BLK // GROUP):
        in_copy(g).start()
    tables[:GRID, :] = row_table[...]
    tables[GRID:, :] = col_table[...]
    label = (keep[...] * (images[...] + 1)).astype(jnp.float32)
    marks[...] = jnp.concatenate([label] * GROUP, axis=1)
    lane = lax.broadcasted_iota(jnp.int32, (SEQ, SEQ), 1)
    line = lax.broadcasted_iota(jnp.int32, (SEQ, SEQ), 0)
    slots = lax.broadcasted_iota(jnp.int32, (SEQ, 2 * GRID), 1).astype(jnp.float32)

    def column(ref, k):
        wide = jnp.broadcast_to(ref[pl.ds(k, 1), :].astype(jnp.float32), (SEQ, SEQ))
        return jnp.sum(jnp.where(lane == line, wide, 0.0), axis=1, keepdims=True)

    def group(g, carry):
        first = g * GROUP
        spots = []
        for j in range(GROUP):
            row, col = column(rows, first + j), column(cols, first + j)
            spots.append(jnp.where((slots == row) | (slots == col + GRID), 1.0, 0.0))
        onehot = jnp.concatenate(spots, axis=0).astype(jnp.bfloat16)
        places = jnp.dot(onehot, tables[...], preferred_element_type=jnp.float32)
        in_copy(g).wait()
        for j in range(GROUP):
            k = first + j
            block = raw[k].astype(jnp.float32) + places[j * SEQ:(j + 1) * SEQ, :]
            block = block.astype(jnp.bfloat16)
            for c in range(COLS):
                buf[k, c * SEQ:(c + 1) * SEQ, :] = block[:, c * 128:(c + 1) * 128]
            mark = jnp.broadcast_to(marks[pl.ds(k, 1), :], (8, 128))
            buf[k, COLS * SEQ:, :] = mark.astype(jnp.bfloat16)
            out_copy(k).start()
        return carry

    lax.fori_loop(0, BLK // GROUP, group, 0)
    for k in range(BLK):
        out_copy(k).wait()


def embed_slots(*operands):
    return pl.pallas_call(
        embed_body,
        out_shape=jax.ShapeDtypeStruct((PEERS, SLOT, 128), jnp.bfloat16),
        in_specs=[SMEM, SMEM] + [VMEM] * 6 + [HBM],
        out_specs=HBM,
        scratch_shapes=[
            pltpu.VMEM((BLK, SLOT, 128), jnp.bfloat16),
            pltpu.VMEM((BLK, SEQ, D), jnp.bfloat16),
            pltpu.VMEM((2 * GRID, D), jnp.bfloat16),
            pltpu.VMEM((BLK, 128), jnp.float32),
            pltpu.SemaphoreType.DMA((BLK // GROUP,)),
            pltpu.SemaphoreType.DMA((BLK,)),
        ],
        compiler_params=pltpu.CompilerParams(vmem_limit_bytes=VMEM_LIMIT),
        name="embed",
    )(*operands)


def sequence(xs, k):
    return jnp.concatenate([xs[k, c * SEQ:(c + 1) * SEQ, :] for c in range(COLS)], axis=1)


def weight_copies(side, own, other, whole, sem, i):
    half = own.shape[0]
    return (
        pltpu.make_async_copy(own, whole.at[pl.ds(side * half, half), :], sem.at[2 * i]),
        pltpu.make_async_copy(
            other, whole.at[pl.ds((1 - side) * half, half), :], sem.at[2 * i + 1]
        ),
    )


def load_sequences(side, order, arrived, sent, xs, sem):
    for k in range(BLK):
        @pl.when(side == 0)
        def _():
            pltpu.make_async_copy(arrived.at[order[k]], xs.at[k], sem.at[k]).start()

        @pl.when(side == 1)
        def _():
            pltpu.make_async_copy(sent.at[k], xs.at[k], sem.at[k]).start()


def await_sequence(sent, xs, sem, k):
    pltpu.make_async_copy(sent.at[k], xs.at[k], sem.at[k]).wait()


def attend_body(
    place, order, arrived, sent, own, other, out,
    xs, w_qkv, normed, qkv, in_sem, w_sem, out_sem,
):
    side = place[1]
    copies = weight_copies(side, own, other, w_qkv, w_sem, 0)

    def out_copy(g):
        part = pl.ds(g * 128, 128)
        return pltpu.make_async_copy(normed.at[part, :], out.at[part, :], out_sem.at[g])

    for copy in copies:
        copy.start()
    load_sequences(side, order, arrived, sent, xs, in_sem)
    for k in range(BLK):
        await_sequence(sent, xs, in_sem, k)

    def first_norm(g, carry):
        for j in range(GROUP):
            k = g * GROUP + j
            x = sequence(xs, k).astype(jnp.float32)
            normed[pl.ds(k * SEQ, SEQ), :] = norm(x).astype(jnp.bfloat16)
        return carry

    lax.fori_loop(0, BLK // GROUP, first_norm, 0)
    for copy in copies:
        copy.wait()

    def project(n, carry):
        for m in range(2):
            part = jnp.dot(
                normed[m * 512:(m + 1) * 512, :], w_qkv[:, pl.ds(n * 512, 512)],
                preferred_element_type=jnp.float32,
            )
            qkv[m * 512:(m + 1) * 512, pl.ds(n * 512, 512)] = part.astype(jnp.bfloat16)
        return carry

    lax.fori_loop(0, 6, project, 0)
    lane = lax.broadcasted_iota(jnp.int32, (128, 128), 1)
    line = lax.broadcasted_iota(jnp.int32, (128, 128), 0)
    low = lane < HEAD_DIM
    zero = jnp.zeros((128, 128), jnp.bfloat16)
    one = jnp.ones((128, 128), jnp.bfloat16)
    ones = jnp.concatenate([jnp.where(low, one, zero), jnp.where(low, zero, one)], axis=0)

    def attend(g, carry):
        base = pl.multiple_of(g * 128, 128)
        label = jnp.zeros((8, 128), jnp.float32)
        for j in range(GROUP):
            marks = xs[g * GROUP + j, COLS * SEQ:, :].astype(jnp.float32)
            label = jnp.where(lane[:8] // SEQ == j, marks, label)
        wide = jnp.broadcast_to(label[:1], (128, 128))
        column = jnp.sum(jnp.where(lane == line, wide, 0.0), axis=1, keepdims=True)
        allowed = (column == wide) & (wide > 0.0) & (lane // SEQ == line // SEQ)
        bias = jnp.where(allowed, 0.0, MASKED)
        bias = jnp.concatenate([bias, bias], axis=0)
        dropped = jnp.where(column == 0.0, 1.0, 0.0)
        for h in range(HEADS // 2):
            q = qkv[pl.ds(base, 128), h * 128:(h + 1) * 128] * jnp.bfloat16(HEAD_DIM ** -0.5)
            key = qkv[pl.ds(base, 128), D + h * 128:D + (h + 1) * 128]
            value = qkv[pl.ds(base, 128), 2 * D + h * 128:2 * D + (h + 1) * 128]
            both = jnp.concatenate([jnp.where(low, q, zero), jnp.where(low, zero, q)], axis=0)
            scores = lax.dot_general(
                both, key, (((1,), (1,)), ((), ())), preferred_element_type=jnp.float32
            )
            scores = scores + bias
            peak = jnp.maximum(jnp.max(scores, axis=1, keepdims=True), 0.1 * MASKED)
            weights = jnp.exp(scores - peak).astype(jnp.bfloat16)
            weights = jnp.concatenate([weights[:128], weights[128:]], axis=1)
            stacked = jnp.concatenate(
                [jnp.where(low, value, zero), jnp.where(low, zero, value)], axis=0
            )
            stacked = jnp.concatenate([stacked, ones], axis=1)
            mixed = jnp.dot(weights, stacked, preferred_element_type=jnp.float32)
            result = mixed[:, :128] / (mixed[:, 128:] + dropped)
            normed[pl.ds(base, 128), h * 128:(h + 1) * 128] = result.astype(jnp.bfloat16)
        out_copy(g).start()
        return carry

    lax.fori_loop(0, BLK // GROUP, attend, 0)
    for g in range(BLK // GROUP):
        out_copy(g).wait()


def attend_kernel(place, order, arrived, sent, own, other):
    bf = jnp.bfloat16
    return pl.pallas_call(
        attend_body,
        out_shape=jax.ShapeDtypeStruct((ROWS, D), bf),
        in_specs=[SMEM, SMEM, HBM, HBM, ANY, ANY],
        out_specs=HBM,
        scratch_shapes=[
            pltpu.VMEM((BLK, SLOT, 128), bf),
            pltpu.VMEM((D, 3 * D), bf),
            pltpu.VMEM((ROWS, D), bf),
            pltpu.VMEM((ROWS, 3 * D), bf),
            pltpu.SemaphoreType.DMA((BLK,)),
            pltpu.SemaphoreType.DMA((2,)),
            pltpu.SemaphoreType.DMA((BLK // GROUP,)),
        ],
        cost_estimate=pl.CostEstimate(
            flops=7_000_000_000, bytes_accessed=12_000_000, transcendentals=2_000_000
        ),
        compiler_params=pltpu.CompilerParams(vmem_limit_bytes=VMEM_LIMIT),
        name="attend",
    )(place, order, arrived, sent, own, other)


def mlp_body(
    place, order, table, attended, arrived, sent, o0, o1, u0, u1, d0, d1, out, results,
    xs, w_out, w_up, w_down, normed, mid, act, outb, live, in_sem, w_sem, out_sem, mix_sem,
):
    me, side = place[0], place[1]
    copies = [
        weight_copies(side, o0, o1, w_out, w_sem, 0),
        weight_copies(side, u0, u1, w_up, w_sem, 1),
        weight_copies(side, d0, d1, w_down, w_sem, 2),
    ]
    mix = pltpu.make_async_copy(attended, normed, mix_sem)
    mix.start()
    for copy in copies[0]:
        copy.start()
    load_sequences(side, order, arrived, sent, xs, in_sem)
    for i in (1, 2):
        for copy in copies[i]:
            copy.start()
    for k in range(BLK):
        await_sequence(sent, xs, in_sem, k)
    lane = lax.broadcasted_iota(jnp.int32, (128, 128), 1)
    line = lax.broadcasted_iota(jnp.int32, (128, 128), 0)

    def alive(g, carry):
        base = pl.multiple_of(g * 128, 128)
        label = jnp.zeros((8, 128), jnp.float32)
        for j in range(GROUP):
            marks = xs[g * GROUP + j, COLS * SEQ:, :].astype(jnp.float32)
            label = jnp.where(lane[:8] // SEQ == j, marks, label)
        wide = jnp.broadcast_to(label[:1], (128, 128))
        column = jnp.sum(jnp.where(lane == line, wide, 0.0), axis=1, keepdims=True)
        live[pl.ds(base, 128), :] = jnp.broadcast_to(column, (128, 128))
        return carry

    lax.fori_loop(0, BLK // GROUP, alive, 0)
    mix.wait()
    for copy in copies[0]:
        copy.wait()

    def merge(m, carry):
        base = pl.multiple_of(m * 256, 256)
        part = jnp.dot(
            normed[pl.ds(base, 256), :], w_out[...], preferred_element_type=jnp.float32
        )
        for j in range(8):
            k = m * 8 + j
            total = sequence(xs, k).astype(jnp.float32) + part[j * SEQ:(j + 1) * SEQ, :]
            mid[pl.ds(k * SEQ, SEQ), :] = total
            normed[pl.ds(k * SEQ, SEQ), :] = norm(total).astype(jnp.bfloat16)
        return carry

    lax.fori_loop(0, 4, merge, 0)
    for copy in copies[1]:
        copy.wait()

    def up(n, carry):
        for m in range(2):
            part = jnp.dot(
                normed[m * 512:(m + 1) * 512, :], w_up[:, pl.ds(n * 512, 512)],
                preferred_element_type=jnp.float32,
            )
            act[m * 512:(m + 1) * 512, pl.ds(n * 512, 512)] = gelu(part).astype(jnp.bfloat16)
        return carry

    lax.fori_loop(0, 8, up, 0)
    for copy in copies[2]:
        copy.wait()

    def down(m, carry):
        base = pl.multiple_of(m * 256, 256)
        part = jnp.dot(act[pl.ds(base, 256), :], w_down[...], preferred_element_type=jnp.float32)
        total = mid[pl.ds(base, 256), :] + part
        total = jnp.where(live[pl.ds(base, 256), :][:, :1] > 0.0, total, 0.0)
        total = total.astype(jnp.bfloat16)
        for j in range(8):
            k = m * 8 + j
            outb[k] = total[j * SEQ:(j + 1) * SEQ, :]

            @pl.when(side == 0)
            def _():
                pltpu.make_async_copy(outb.at[k], out.at[k], out_sem.at[k]).start()

            @pl.when(side == 1)
            def _():
                pltpu.make_async_copy(
                    outb.at[k], results.at[table[0, me, k]], out_sem.at[k]
                ).start()
        return carry

    lax.fori_loop(0, 4, down, 0)
    for k in range(BLK):
        pltpu.make_async_copy(outb.at[k], out.at[k], out_sem.at[k]).wait()


def mlp_kernel(*operands):
    bf, f32 = jnp.bfloat16, jnp.float32
    return pl.pallas_call(
        mlp_body,
        out_shape=(
            jax.ShapeDtypeStruct((BLK, SEQ, D), bf),
            jax.ShapeDtypeStruct((PEERS, SEQ, D), bf),
        ),
        in_specs=[SMEM, SMEM, SMEM] + [HBM] * 9,
        out_specs=(HBM, HBM),
        scratch_shapes=[
            pltpu.VMEM((BLK, SLOT, 128), bf),
            pltpu.VMEM((D, D), bf),
            pltpu.VMEM((D, MLP), bf),
            pltpu.VMEM((MLP, D), bf),
            pltpu.VMEM((ROWS, D), bf),
            pltpu.VMEM((ROWS, D), f32),
            pltpu.VMEM((ROWS, MLP), bf),
            pltpu.VMEM((BLK, SEQ, D), bf),
            pltpu.VMEM((ROWS, 128), f32),
            pltpu.SemaphoreType.DMA((BLK,)),
            pltpu.SemaphoreType.DMA((6,)),
            pltpu.SemaphoreType.DMA((BLK,)),
            pltpu.SemaphoreType.DMA,
        ],
        cost_estimate=pl.CostEstimate(
            flops=20_000_000_000, bytes_accessed=25_000_000, transcendentals=4_000_000
        ),
        compiler_params=pltpu.CompilerParams(vmem_limit_bytes=VMEM_LIMIT),
        name="mlp",
    )(*operands)


def settle_body(place, order, returned, out_in, out, sem):
    @pl.when(place[1] == 1)
    def _():
        for k in range(BLK):
            pltpu.make_async_copy(returned.at[order[k]], out.at[k], sem.at[k]).start()
        for k in range(BLK):
            pltpu.make_async_copy(returned.at[order[k]], out.at[k], sem.at[k]).wait()


def settle_kernel(place, order, returned, out):
    return pl.pallas_call(
        settle_body,
        out_shape=jax.ShapeDtypeStruct(out.shape, out.dtype),
        in_specs=[SMEM, SMEM, HBM, HBM],
        out_specs=HBM,
        scratch_shapes=[pltpu.SemaphoreType.DMA((BLK,))],
        input_output_aliases={3: 0},
        name="settle",
    )(place, order, returned, out)


def blank(like):
    return pl.pallas_call(
        lambda ref, out: None,
        out_shape=jax.ShapeDtypeStruct(like.shape, like.dtype),
        in_specs=[HBM],
        out_specs=HBM,
        name="blank",
    )(like)


def exchange(chosen, values):
    return lax.cond(
        chosen,
        lambda x: lax.all_to_all(x, "dp", split_axis=0, concat_axis=0, tiled=True),
        blank,
        values,
    )


def arrivals(table, myself):
    filled = jnp.any(table == myself, axis=1)
    places = jnp.arange(PEERS, dtype=jnp.int32)
    rank = jnp.sum((filled[None, :] & (places[None, :] < places[:, None])).astype(jnp.int32), axis=1)
    wanted = jnp.arange(BLK, dtype=jnp.int32)
    hit = filled[None, :] & (rank[None, :] == wanted[:, None])
    return jnp.sum(jnp.where(hit, places[None, :], 0), axis=1)


def local(
    patches, rows, cols, keep, images, destination, row_table, col_table, w_qkv, w_out, w_up, w_down
):
    myself = lax.axis_index("dp").astype(jnp.int32)
    side = lax.axis_index("fsdp").astype(jnp.int32)
    place = jnp.stack([myself, side])
    swap = [(0, 1), (1, 0)]
    pairs = []
    for w in (w_qkv, w_out, w_up, w_down):
        pairs.append((w, lax.ppermute(w, "fsdp", swap)))
    sent = embed_slots(
        place, destination, rows, cols, keep, images, row_table, col_table, patches
    )
    order = arrivals(destination[0], myself)
    arrived = exchange(side == 0, sent)
    attended = attend_kernel(place, order, arrived, sent, *pairs[0])
    out, results = mlp_kernel(
        place, order, destination, attended, arrived, sent, *pairs[1], *pairs[2], *pairs[3]
    )
    returned = exchange(side == 1, results)
    return settle_kernel(place, order, returned, out)


def solution(mesh):
    whole = P(("dp", "fsdp"), None, None)
    flat = P(("dp", "fsdp"), None)
    half = P("fsdp", None)
    in_specs = (
        whole, flat, flat, flat, flat, P("fsdp", None, None), P(), P(), half, half, half, half,
    )
    return jax.shard_map(local, mesh=mesh, in_specs=in_specs, out_specs=whole, check_vma=False)
```

```python
import jax
import jax.numpy as jnp
from jax import lax
from jax.experimental import pallas as pl
from jax.experimental.pallas import tpu as pltpu
from jax.sharding import PartitionSpec as P


HEADS = 16
HEAD_DIM = 64
BLK = 32
SEQ = 32
D = 1024
MLP = 4096
PEERS = 64
GRID = 64
ROWS = BLK * SEQ
COLS = D // 128
SLOT = COLS * SEQ + 8
GROUP = 4
EPS = 1e-06
MASKED = -1e30
VMEM_LIMIT = 60 * 1024 * 1024
ANY = pl.BlockSpec(memory_space=pl.ANY)
HBM = pl.BlockSpec(memory_space=pltpu.HBM)
SMEM = pl.BlockSpec(memory_space=pltpu.SMEM)
VMEM = pl.BlockSpec(memory_space=pltpu.VMEM)


def norm(values):
    center = values - jnp.mean(values, axis=-1, keepdims=True)
    spread = jnp.mean(center * center, axis=-1, keepdims=True)
    return center * lax.rsqrt(spread + EPS)


def gelu(x):
    inner = x * (0.7978845608028654 + 0.035677408136300125 * (x * x))
    half = 0.5 * x
    return half + half * jnp.tanh(inner)


def embed_body(
    place, table, rows, cols, keep, images, row_table, col_table, patches, out,
    buf, raw, tables, marks, in_sem, sem,
):
    me, side = place[0], place[1]

    def in_copy(g):
        part = pl.ds(g * GROUP, GROUP)
        return pltpu.make_async_copy(patches.at[part], raw.at[part], in_sem.at[g])

    def out_copy(k):
        slot = jnp.where(side == 0, table[0, me, k], k)
        return pltpu.make_async_copy(buf.at[k], out.at[slot], sem.at[k])

    for g in range(BLK // GROUP):
        in_copy(g).start()
    tables[:GRID, :] = row_table[...]
    tables[GRID:, :] = col_table[...]
    label = (keep[...] * (images[...] + 1)).astype(jnp.float32)
    marks[...] = jnp.concatenate([label] * GROUP, axis=1)
    lane = lax.broadcasted_iota(jnp.int32, (SEQ, SEQ), 1)
    line = lax.broadcasted_iota(jnp.int32, (SEQ, SEQ), 0)
    slots = lax.broadcasted_iota(jnp.int32, (SEQ, 2 * GRID), 1).astype(jnp.float32)

    def column(ref, k):
        wide = jnp.broadcast_to(ref[pl.ds(k, 1), :].astype(jnp.float32), (SEQ, SEQ))
        return jnp.sum(jnp.where(lane == line, wide, 0.0), axis=1, keepdims=True)

    def group(g, carry):
        first = g * GROUP
        spots = []
        for j in range(GROUP):
            row, col = column(rows, first + j), column(cols, first + j)
            spots.append(jnp.where((slots == row) | (slots == col + GRID), 1.0, 0.0))
        onehot = jnp.concatenate(spots, axis=0).astype(jnp.bfloat16)
        places = jnp.dot(onehot, tables[...], preferred_element_type=jnp.float32)
        in_copy(g).wait()
        for j in range(GROUP):
            k = first + j
            block = raw[k].astype(jnp.float32) + places[j * SEQ:(j + 1) * SEQ, :]
            block = block.astype(jnp.bfloat16)
            for c in range(COLS):
                buf[k, c * SEQ:(c + 1) * SEQ, :] = block[:, c * 128:(c + 1) * 128]
            mark = jnp.broadcast_to(marks[pl.ds(k, 1), :], (8, 128))
            buf[k, COLS * SEQ:, :] = mark.astype(jnp.bfloat16)
            out_copy(k).start()
        return carry

    lax.fori_loop(0, BLK // GROUP, group, 0)
    for k in range(BLK):
        out_copy(k).wait()


def embed_slots(*operands):
    return pl.pallas_call(
        embed_body,
        out_shape=jax.ShapeDtypeStruct((PEERS, SLOT, 128), jnp.bfloat16),
        in_specs=[SMEM, SMEM] + [VMEM] * 6 + [HBM],
        out_specs=HBM,
        scratch_shapes=[
            pltpu.VMEM((BLK, SLOT, 128), jnp.bfloat16),
            pltpu.VMEM((BLK, SEQ, D), jnp.bfloat16),
            pltpu.VMEM((2 * GRID, D), jnp.bfloat16),
            pltpu.VMEM((BLK, 128), jnp.float32),
            pltpu.SemaphoreType.DMA((BLK // GROUP,)),
            pltpu.SemaphoreType.DMA((BLK,)),
        ],
        compiler_params=pltpu.CompilerParams(vmem_limit_bytes=VMEM_LIMIT),
        name="embed",
    )(*operands)


def sequence(xs, k):
    return jnp.concatenate([xs[k, c * SEQ:(c + 1) * SEQ, :] for c in range(COLS)], axis=1)


def weight_copies(side, own, other, whole, sem, i):
    half = own.shape[0]
    return (
        pltpu.make_async_copy(own, whole.at[pl.ds(side * half, half), :], sem.at[2 * i]),
        pltpu.make_async_copy(
            other, whole.at[pl.ds((1 - side) * half, half), :], sem.at[2 * i + 1]
        ),
    )


def load_sequences(side, order, arrived, sent, xs, sem):
    for k in range(BLK):
        @pl.when(side == 0)
        def _():
            pltpu.make_async_copy(arrived.at[order[k]], xs.at[k], sem.at[k]).start()

        @pl.when(side == 1)
        def _():
            pltpu.make_async_copy(sent.at[k], xs.at[k], sem.at[k]).start()


def await_sequence(sent, xs, sem, k):
    pltpu.make_async_copy(sent.at[k], xs.at[k], sem.at[k]).wait()


def attend_body(
    place, order, arrived, sent, own, other, out,
    xs, w_qkv, normed, qkv, in_sem, w_sem, out_sem,
):
    side = place[1]
    copies = weight_copies(side, own, other, w_qkv, w_sem, 0)

    def out_copy(g):
        part = pl.ds(g * 128, 128)
        return pltpu.make_async_copy(normed.at[part, :], out.at[part, :], out_sem.at[g])

    for copy in copies:
        copy.start()
    load_sequences(side, order, arrived, sent, xs, in_sem)
    for k in range(BLK):
        await_sequence(sent, xs, in_sem, k)

    def first_norm(g, carry):
        for j in range(GROUP):
            k = g * GROUP + j
            x = sequence(xs, k).astype(jnp.float32)
            normed[pl.ds(k * SEQ, SEQ), :] = norm(x).astype(jnp.bfloat16)
        return carry

    lax.fori_loop(0, BLK // GROUP, first_norm, 0)
    for copy in copies:
        copy.wait()

    def project(n, carry):
        for m in range(2):
            part = jnp.dot(
                normed[m * 512:(m + 1) * 512, :], w_qkv[:, pl.ds(n * 512, 512)],
                preferred_element_type=jnp.float32,
            )
            qkv[m * 512:(m + 1) * 512, pl.ds(n * 512, 512)] = part.astype(jnp.bfloat16)
        return carry

    lax.fori_loop(0, 6, project, 0)
    lane = lax.broadcasted_iota(jnp.int32, (128, 128), 1)
    line = lax.broadcasted_iota(jnp.int32, (128, 128), 0)
    low = lane < HEAD_DIM
    zero = jnp.zeros((128, 128), jnp.bfloat16)
    one = jnp.ones((128, 128), jnp.bfloat16)
    ones = jnp.concatenate([jnp.where(low, one, zero), jnp.where(low, zero, one)], axis=0)

    def attend(g, carry):
        base = pl.multiple_of(g * 128, 128)
        label = jnp.zeros((8, 128), jnp.float32)
        for j in range(GROUP):
            marks = xs[g * GROUP + j, COLS * SEQ:, :].astype(jnp.float32)
            label = jnp.where(lane[:8] // SEQ == j, marks, label)
        wide = jnp.broadcast_to(label[:1], (128, 128))
        column = jnp.sum(jnp.where(lane == line, wide, 0.0), axis=1, keepdims=True)
        allowed = (column == wide) & (wide > 0.0) & (lane // SEQ == line // SEQ)
        bias = jnp.where(allowed, 0.0, MASKED)
        bias = jnp.concatenate([bias, bias], axis=0)
        dropped = jnp.where(column == 0.0, 1.0, 0.0)
        for h in range(HEADS // 2):
            q = qkv[pl.ds(base, 128), h * 128:(h + 1) * 128] * jnp.bfloat16(HEAD_DIM ** -0.5)
            key = qkv[pl.ds(base, 128), D + h * 128:D + (h + 1) * 128]
            value = qkv[pl.ds(base, 128), 2 * D + h * 128:2 * D + (h + 1) * 128]
            both = jnp.concatenate([jnp.where(low, q, zero), jnp.where(low, zero, q)], axis=0)
            scores = lax.dot_general(
                both, key, (((1,), (1,)), ((), ())), preferred_element_type=jnp.float32
            )
            scores = scores + bias
            peak = jnp.maximum(jnp.max(scores, axis=1, keepdims=True), 0.1 * MASKED)
            weights = jnp.exp(scores - peak).astype(jnp.bfloat16)
            weights = jnp.concatenate([weights[:128], weights[128:]], axis=1)
            stacked = jnp.concatenate(
                [jnp.where(low, value, zero), jnp.where(low, zero, value)], axis=0
            )
            stacked = jnp.concatenate([stacked, ones], axis=1)
            mixed = jnp.dot(weights, stacked, preferred_element_type=jnp.float32)
            result = mixed[:, :128] / (mixed[:, 128:] + dropped)
            normed[pl.ds(base, 128), h * 128:(h + 1) * 128] = result.astype(jnp.bfloat16)
        out_copy(g).start()
        return carry

    lax.fori_loop(0, BLK // GROUP, attend, 0)
    for g in range(BLK // GROUP):
        out_copy(g).wait()


def attend_kernel(place, order, arrived, sent, own, other):
    bf = jnp.bfloat16
    return pl.pallas_call(
        attend_body,
        out_shape=jax.ShapeDtypeStruct((ROWS, D), bf),
        in_specs=[SMEM, SMEM, HBM, HBM, ANY, ANY],
        out_specs=HBM,
        scratch_shapes=[
            pltpu.VMEM((BLK, SLOT, 128), bf),
            pltpu.VMEM((D, 3 * D), bf),
            pltpu.VMEM((ROWS, D), bf),
            pltpu.VMEM((ROWS, 3 * D), bf),
            pltpu.SemaphoreType.DMA((BLK,)),
            pltpu.SemaphoreType.DMA((2,)),
            pltpu.SemaphoreType.DMA((BLK // GROUP,)),
        ],
        cost_estimate=pl.CostEstimate(
            flops=7_000_000_000, bytes_accessed=12_000_000, transcendentals=2_000_000
        ),
        compiler_params=pltpu.CompilerParams(vmem_limit_bytes=VMEM_LIMIT),
        name="attend",
    )(place, order, arrived, sent, own, other)


def mlp_body(
    place, order, table, attended, arrived, sent, o0, o1, u0, u1, d0, d1, out, results,
    xs, w_out, w_up, w_down, normed, mid, act, outb, live, in_sem, w_sem, out_sem, mix_sem,
):
    me, side = place[0], place[1]
    copies = [
        weight_copies(side, o0, o1, w_out, w_sem, 0),
        weight_copies(side, u0, u1, w_up, w_sem, 1),
        weight_copies(side, d0, d1, w_down, w_sem, 2),
    ]
    mix = pltpu.make_async_copy(attended, normed, mix_sem)
    mix.start()
    for copy in copies[0]:
        copy.start()
    load_sequences(side, order, arrived, sent, xs, in_sem)
    for i in (1, 2):
        for copy in copies[i]:
            copy.start()
    for k in range(BLK):
        await_sequence(sent, xs, in_sem, k)
    lane = lax.broadcasted_iota(jnp.int32, (128, 128), 1)
    line = lax.broadcasted_iota(jnp.int32, (128, 128), 0)

    def alive(g, carry):
        base = pl.multiple_of(g * 128, 128)
        label = jnp.zeros((8, 128), jnp.float32)
        for j in range(GROUP):
            marks = xs[g * GROUP + j, COLS * SEQ:, :].astype(jnp.float32)
            label = jnp.where(lane[:8] // SEQ == j, marks, label)
        wide = jnp.broadcast_to(label[:1], (128, 128))
        column = jnp.sum(jnp.where(lane == line, wide, 0.0), axis=1, keepdims=True)
        live[pl.ds(base, 128), :] = jnp.broadcast_to(column, (128, 128))
        return carry

    lax.fori_loop(0, BLK // GROUP, alive, 0)
    mix.wait()
    for copy in copies[0]:
        copy.wait()

    def merge(m, carry):
        base = pl.multiple_of(m * 256, 256)
        part = jnp.dot(
            normed[pl.ds(base, 256), :], w_out[...], preferred_element_type=jnp.float32
        )
        for j in range(8):
            k = m * 8 + j
            total = sequence(xs, k).astype(jnp.float32) + part[j * SEQ:(j + 1) * SEQ, :]
            mid[pl.ds(k * SEQ, SEQ), :] = total
            normed[pl.ds(k * SEQ, SEQ), :] = norm(total).astype(jnp.bfloat16)
        return carry

    lax.fori_loop(0, 4, merge, 0)
    for copy in copies[1]:
        copy.wait()

    def up(n, carry):
        for m in range(2):
            part = jnp.dot(
                normed[m * 512:(m + 1) * 512, :], w_up[:, pl.ds(n * 512, 512)],
                preferred_element_type=jnp.float32,
            )
            act[m * 512:(m + 1) * 512, pl.ds(n * 512, 512)] = gelu(part).astype(jnp.bfloat16)
        return carry

    lax.fori_loop(0, 8, up, 0)
    for copy in copies[2]:
        copy.wait()

    def down(m, carry):
        base = pl.multiple_of(m * 256, 256)
        part = jnp.dot(act[pl.ds(base, 256), :], w_down[...], preferred_element_type=jnp.float32)
        total = mid[pl.ds(base, 256), :] + part
        total = jnp.where(live[pl.ds(base, 256), :][:, :1] > 0.0, total, 0.0)
        total = total.astype(jnp.bfloat16)
        for j in range(8):
            k = m * 8 + j
            outb[k] = total[j * SEQ:(j + 1) * SEQ, :]

            @pl.when(side == 0)
            def _():
                pltpu.make_async_copy(outb.at[k], out.at[k], out_sem.at[k]).start()

            @pl.when(side == 1)
            def _():
                pltpu.make_async_copy(
                    outb.at[k], results.at[table[0, me, k]], out_sem.at[k]
                ).start()
        return carry

    lax.fori_loop(0, 4, down, 0)
    for k in range(BLK):
        pltpu.make_async_copy(outb.at[k], out.at[k], out_sem.at[k]).wait()


def mlp_kernel(*operands):
    bf, f32 = jnp.bfloat16, jnp.float32
    return pl.pallas_call(
        mlp_body,
        out_shape=(
            jax.ShapeDtypeStruct((BLK, SEQ, D), bf),
            jax.ShapeDtypeStruct((PEERS, SEQ, D), bf),
        ),
        in_specs=[SMEM, SMEM, SMEM] + [HBM] * 9,
        out_specs=(HBM, HBM),
        scratch_shapes=[
            pltpu.VMEM((BLK, SLOT, 128), bf),
            pltpu.VMEM((D, D), bf),
            pltpu.VMEM((D, MLP), bf),
            pltpu.VMEM((MLP, D), bf),
            pltpu.VMEM((ROWS, D), bf),
            pltpu.VMEM((ROWS, D), f32),
            pltpu.VMEM((ROWS, MLP), bf),
            pltpu.VMEM((BLK, SEQ, D), bf),
            pltpu.VMEM((ROWS, 128), f32),
            pltpu.SemaphoreType.DMA((BLK,)),
            pltpu.SemaphoreType.DMA((6,)),
            pltpu.SemaphoreType.DMA((BLK,)),
            pltpu.SemaphoreType.DMA,
        ],
        cost_estimate=pl.CostEstimate(
            flops=20_000_000_000, bytes_accessed=25_000_000, transcendentals=4_000_000
        ),
        compiler_params=pltpu.CompilerParams(vmem_limit_bytes=VMEM_LIMIT),
        name="mlp",
    )(*operands)


def settle_body(place, order, returned, out_in, out, buf, in_sem, out_sem):
    def in_copy(k):
        return pltpu.make_async_copy(returned.at[order[k]], buf.at[k], in_sem.at[k])

    def out_copy(k):
        return pltpu.make_async_copy(buf.at[k], out.at[k], out_sem.at[k])

    @pl.when(place[1] == 1)
    def _():
        for k in range(BLK):
            in_copy(k).start()
        for k in range(BLK):
            in_copy(k).wait()
            out_copy(k).start()
        for k in range(BLK):
            out_copy(k).wait()


def settle_kernel(place, order, returned, out):
    return pl.pallas_call(
        settle_body,
        out_shape=jax.ShapeDtypeStruct(out.shape, out.dtype),
        in_specs=[SMEM, SMEM, HBM, HBM],
        out_specs=HBM,
        scratch_shapes=[
            pltpu.VMEM((BLK, SEQ, D), jnp.bfloat16),
            pltpu.SemaphoreType.DMA((BLK,)),
            pltpu.SemaphoreType.DMA((BLK,)),
        ],
        input_output_aliases={3: 0},
        compiler_params=pltpu.CompilerParams(vmem_limit_bytes=VMEM_LIMIT),
        name="settle",
    )(place, order, returned, out)


def blank(like):
    return pl.pallas_call(
        lambda ref, out: None,
        out_shape=jax.ShapeDtypeStruct(like.shape, like.dtype),
        in_specs=[HBM],
        out_specs=HBM,
        name="blank",
    )(like)


def exchange(chosen, values):
    return lax.cond(
        chosen,
        lambda x: lax.all_to_all(x, "dp", split_axis=0, concat_axis=0, tiled=True),
        blank,
        values,
    )


def arrivals(table, myself):
    filled = jnp.any(table == myself, axis=1)
    places = jnp.arange(PEERS, dtype=jnp.int32)
    rank = jnp.sum((filled[None, :] & (places[None, :] < places[:, None])).astype(jnp.int32), axis=1)
    wanted = jnp.arange(BLK, dtype=jnp.int32)
    hit = filled[None, :] & (rank[None, :] == wanted[:, None])
    return jnp.sum(jnp.where(hit, places[None, :], 0), axis=1)


def local(
    patches, rows, cols, keep, images, destination, row_table, col_table, w_qkv, w_out, w_up, w_down
):
    myself = lax.axis_index("dp").astype(jnp.int32)
    side = lax.axis_index("fsdp").astype(jnp.int32)
    place = jnp.stack([myself, side])
    swap = [(0, 1), (1, 0)]
    pairs = []
    for w in (w_qkv, w_out, w_up, w_down):
        pairs.append((w, lax.ppermute(w, "fsdp", swap)))
    sent = embed_slots(
        place, destination, rows, cols, keep, images, row_table, col_table, patches
    )
    order = arrivals(destination[0], myself)
    arrived = exchange(side == 0, sent)
    attended = attend_kernel(place, order, arrived, sent, *pairs[0])
    out, results = mlp_kernel(
        place, order, destination, attended, arrived, sent, *pairs[1], *pairs[2], *pairs[3]
    )
    returned = exchange(side == 1, results)
    return settle_kernel(place, order, returned, out)


def solution(mesh):
    whole = P(("dp", "fsdp"), None, None)
    flat = P(("dp", "fsdp"), None)
    half = P("fsdp", None)
    in_specs = (
        whole, flat, flat, flat, flat, P("fsdp", None, None), P(), P(), half, half, half, half,
    )
    return jax.shard_map(local, mesh=mesh, in_specs=in_specs, out_specs=whole, check_vma=False)
```

```python
import jax
import jax.numpy as jnp
from jax import lax
from jax.experimental import pallas as pl
from jax.experimental.pallas import tpu as pltpu
from jax.sharding import PartitionSpec as P


HEADS = 16
HEAD_DIM = 64
BLK = 32
SEQ = 32
D = 1024
MLP = 4096
PEERS = 64
GRID = 64
ROWS = BLK * SEQ
COLS = D // 128
SLOT = COLS * SEQ + 8
GROUP = 4
EPS = 1e-06
UP = 512
DOWN = 256
MASKED = -1e30
VMEM_LIMIT = 60 * 1024 * 1024
ATTEND_LIMIT = 36 * 1024 * 1024
WIDE = 512
ANY = pl.BlockSpec(memory_space=pl.ANY)
HBM = pl.BlockSpec(memory_space=pltpu.HBM)
SMEM = pl.BlockSpec(memory_space=pltpu.SMEM)
VMEM = pl.BlockSpec(memory_space=pltpu.VMEM)


def norm(values):
    center = values - jnp.mean(values, axis=-1, keepdims=True)
    spread = jnp.mean(center * center, axis=-1, keepdims=True)
    return center * lax.rsqrt(spread + EPS)


def gelu(x):
    inner = x * (0.7978845608028654 + 0.035677408136300125 * (x * x))
    half = 0.5 * x
    return half + half * jnp.tanh(inner)


def embed_body(
    table, wide_table, rows, cols, keep, images, row_table, col_table, patches, out, order,
    buf, raw, tables, marks, spots, in_sem, sem,
):
    me, side = lax.axis_index("dp"), lax.axis_index("fsdp")

    def in_copy(g):
        part = pl.ds(g * 2 * GROUP, 2 * GROUP)
        return pltpu.make_async_copy(patches.at[part], raw.at[part], in_sem.at[g])

    def out_copy(k):
        slot = jnp.where(side == 0, table[0, k, me], k)
        return pltpu.make_async_copy(buf.at[k], out.at[slot], sem.at[k])

    for g in range(BLK // GROUP // 2):
        in_copy(g).start()
    tables[:GRID, :] = row_table[...]
    tables[GRID:, :] = col_table[...]
    label = (keep[...] * (images[...] + 1)).astype(jnp.float32)
    marks[...] = jnp.concatenate([label] * GROUP, axis=1)
    for i, ref in enumerate((rows, cols)):
        parts = [ref[pl.ds(j, BLK // GROUP, stride=GROUP), :] for j in range(GROUP)]
        spots[i] = jnp.concatenate(parts, axis=1)
    slots = lax.broadcasted_iota(jnp.int32, (2 * GRID, 128), 0)
    for g in range(BLK // GROUP):
        row, col = spots[0, g:g + 1, :], spots[1, g:g + 1, :] + GRID
        onehot = jnp.where((slots == row) | (slots == col), 1.0, 0.0).astype(jnp.bfloat16)
        places = lax.dot_general(
            onehot, tables[...], (((0,), (0,)), ((), ())), preferred_element_type=jnp.float32
        )
        if g % 2 == 0:
            in_copy(g // 2).wait()
        for j in range(GROUP):
            k = g * GROUP + j
            block = raw[k].astype(jnp.float32) + places[j * SEQ:(j + 1) * SEQ, :]
            block = block.astype(jnp.bfloat16)
            for c in range(COLS):
                buf[k, c * SEQ:(c + 1) * SEQ, :] = block[:, c * 128:(c + 1) * 128]
            mark = jnp.broadcast_to(marks[k:k + 1, :], (8, 128))
            buf[k, COLS * SEQ:, :] = mark.astype(jnp.bfloat16)
            out_copy(k).start()
    hits = jnp.where(wide_table[0] == me, 1.0, 0.0)
    filled = jnp.broadcast_to(jnp.max(hits, axis=0, keepdims=True), (BLK, PEERS))
    before = lax.broadcasted_iota(jnp.int32, (PEERS, PEERS), 0)
    after = lax.broadcasted_iota(jnp.int32, (PEERS, PEERS), 1)
    earlier = jnp.where(before < after, 1.0, 0.0).astype(jnp.bfloat16)
    rank = jnp.dot(filled.astype(jnp.bfloat16), earlier, preferred_element_type=jnp.float32)
    wanted = lax.broadcasted_iota(jnp.int32, (BLK, PEERS), 0).astype(jnp.float32)
    source = lax.broadcasted_iota(jnp.int32, (BLK, PEERS), 1).astype(jnp.float32)
    picked = jnp.where((filled > 0.0) & (rank == wanted), source, 0.0)
    picked = jnp.sum(picked, axis=1, keepdims=True)
    order[...] = jnp.broadcast_to(picked, (BLK, 128)).astype(jnp.int32)
    for k in range(BLK):
        out_copy(k).wait()


def embed_slots(*operands):
    return pl.pallas_call(
        embed_body,
        out_shape=(
            jax.ShapeDtypeStruct((PEERS, SLOT, 128), jnp.bfloat16),
            jax.ShapeDtypeStruct((BLK, 128), jnp.int32),
        ),
        in_specs=[SMEM] + [VMEM] * 7 + [HBM],
        out_specs=(HBM, VMEM),
        scratch_shapes=[
            pltpu.VMEM((BLK, SLOT, 128), jnp.bfloat16),
            pltpu.VMEM((BLK, SEQ, D), jnp.bfloat16),
            pltpu.VMEM((2 * GRID, D), jnp.bfloat16),
            pltpu.VMEM((BLK, 128), jnp.float32),
            pltpu.VMEM((2, BLK // GROUP, 128), jnp.int32),
            pltpu.SemaphoreType.DMA((BLK // GROUP // 2,)),
            pltpu.SemaphoreType.DMA((BLK,)),
        ],
        compiler_params=pltpu.CompilerParams(vmem_limit_bytes=VMEM_LIMIT),
        name="embed",
    )(*operands)


def sequence(xs, k):
    return jnp.concatenate([xs[k, c * SEQ:(c + 1) * SEQ, :] for c in range(COLS)], axis=1)


def weight_copies(side, own, other, whole, sem):
    half = own.shape[0]
    return [
        pltpu.make_async_copy(piece, whole.at[pl.ds(row * half, half), :], sem.at[i])
        for i, (piece, row) in enumerate(((own, side), (other, 1 - side)))
    ]


def run(copies, act):
    for copy in copies:
        getattr(copy, act)()


def marks_of(xs, g):
    lane = lax.broadcasted_iota(jnp.int32, (128, 128), 1)
    line = lax.broadcasted_iota(jnp.int32, (128, 128), 0)
    label = jnp.zeros((8, 128), jnp.float32)
    for j in range(GROUP):
        marks = xs[g * GROUP + j, COLS * SEQ:, :].astype(jnp.float32)
        label = jnp.where(lane[:8] // SEQ == j, marks, label)
    wide = jnp.broadcast_to(label[:1], (128, 128))
    column = jnp.sum(jnp.where(lane == line, wide, 0.0), axis=1, keepdims=True)
    return wide, column


def load_sequences(side, order, arrived, sent, xs, sem, low, high):
    for k in range(low, high):
        @pl.when(side == 0)
        def _():
            pltpu.make_async_copy(arrived.at[order[k, 0]], xs.at[k], sem.at[k]).start()

        @pl.when(side == 1)
        def _():
            pltpu.make_async_copy(sent.at[k], xs.at[k], sem.at[k]).start()


def await_sequence(sent, xs, sem, k):
    pltpu.make_async_copy(sent.at[k], xs.at[k], sem.at[k]).wait()


def attend_body(
    order, arrived, sent, own, other, out,
    xs, w_qkv, normed, qkv, mixed, in_sem, w_sem, out_sem,
):
    side = lax.axis_index("fsdp")
    copies = weight_copies(side, own, other, w_qkv, w_sem.at[0])

    def out_copy(g):
        part = pl.ds(g * 128, 128)
        return pltpu.make_async_copy(mixed.at[part, :], out.at[part, :], out_sem.at[g])

    load_sequences(side, order, arrived, sent, xs, in_sem, 0, 8)
    run(copies, "start")
    load_sequences(side, order, arrived, sent, xs, in_sem, 8, BLK)

    def smooth(m, slot):
        for j in range(8):
            x = sequence(xs, m * 8 + j).astype(jnp.float32)
            normed[slot, j * SEQ:(j + 1) * SEQ, :] = norm(x).astype(jnp.bfloat16)

    def project(m, slot):
        base = m * 256 if isinstance(m, int) else pl.multiple_of(m * 256, 256)
        for n in range(3 * D // WIDE):
            part = jnp.dot(
                normed[slot], w_qkv[:, n * WIDE:(n + 1) * WIDE],
                preferred_element_type=jnp.float32,
            )
            qkv[pl.ds(base, 256), n * WIDE:(n + 1) * WIDE] = part.astype(jnp.bfloat16)

    for j in range(8):
        await_sequence(sent, xs, in_sem, j)
    smooth(0, 0)
    for j in range(8, BLK):
        await_sequence(sent, xs, in_sem, j)
    run(copies, "wait")

    def block(m, carry):
        slot = m % 2
        project(m, slot)
        smooth(m + 1, 1 - slot)
        return carry

    lax.fori_loop(0, 3, block, 0)
    project(3, 1)
    lane = lax.broadcasted_iota(jnp.int32, (128, 128), 1)
    line = lax.broadcasted_iota(jnp.int32, (128, 128), 0)
    low = lane < HEAD_DIM
    zero = jnp.zeros((128, 128), jnp.bfloat16)
    one = jnp.ones((128, 128), jnp.bfloat16)
    ones = jnp.concatenate([jnp.where(low, one, zero), jnp.where(low, zero, one)], axis=0)

    def attend(g, carry):
        base = pl.multiple_of(g * 128, 128)
        wide, column = marks_of(xs, g)
        allowed = (column == wide) & (wide > 0.0) & (lane // SEQ == line // SEQ)
        bias = jnp.where(allowed, 0.0, MASKED)
        bias = jnp.concatenate([bias, bias], axis=0)
        dropped = jnp.where(column == 0.0, 1.0, 0.0)
        for h in range(HEADS // 2):
            q = qkv[pl.ds(base, 128), h * 128:(h + 1) * 128] * jnp.bfloat16(HEAD_DIM ** -0.5)
            key = qkv[pl.ds(base, 128), D + h * 128:D + (h + 1) * 128]
            value = qkv[pl.ds(base, 128), 2 * D + h * 128:2 * D + (h + 1) * 128]
            both = jnp.concatenate([jnp.where(low, q, zero), jnp.where(low, zero, q)], axis=0)
            scores = lax.dot_general(
                both, key, (((1,), (1,)), ((), ())), preferred_element_type=jnp.float32
            )
            scores = scores + bias
            peak = jnp.maximum(jnp.max(scores, axis=1, keepdims=True), 0.1 * MASKED)
            weights = jnp.exp(scores - peak).astype(jnp.bfloat16)
            weights = jnp.concatenate([weights[:128], weights[128:]], axis=1)
            stacked = jnp.concatenate(
                [jnp.where(low, value, zero), jnp.where(low, zero, value)], axis=0
            )
            stacked = jnp.concatenate([stacked, ones], axis=1)
            both = jnp.dot(weights, stacked, preferred_element_type=jnp.float32)
            result = both[:, :128] / (both[:, 128:] + dropped)
            mixed[pl.ds(base, 128), h * 128:(h + 1) * 128] = result.astype(jnp.bfloat16)
        out_copy(g).start()
        return carry

    lax.fori_loop(0, BLK // GROUP, attend, 0)
    for g in range(BLK // GROUP):
        out_copy(g).wait()


def attend_kernel(order, arrived, sent, own, other):
    bf = jnp.bfloat16
    return pl.pallas_call(
        attend_body,
        out_shape=jax.ShapeDtypeStruct((ROWS, D), bf),
        in_specs=[SMEM, HBM, HBM, ANY, ANY],
        out_specs=HBM,
        scratch_shapes=[
            pltpu.VMEM((BLK, SLOT, 128), bf),
            pltpu.VMEM((D, 3 * D), bf),
            pltpu.VMEM((2, 256, D), bf),
            pltpu.VMEM((ROWS, 3 * D), bf),
            pltpu.VMEM((ROWS, D), bf),
            pltpu.SemaphoreType.DMA((BLK,)),
            pltpu.SemaphoreType.DMA((1, 2)),
            pltpu.SemaphoreType.DMA((BLK // GROUP,)),
        ],
        cost_estimate=pl.CostEstimate(
            flops=7_000_000_000, bytes_accessed=12_000_000, transcendentals=2_000_000
        ),
        compiler_params=pltpu.CompilerParams(vmem_limit_bytes=ATTEND_LIMIT),
        name="attend",
    )(order, arrived, sent, own, other)


def mlp_body(
    order, table, attended, arrived, sent, o0, o1, u0, u1, d0, d1, out, results,
    xs, w_out, w_up, w_down, normed, second, mid, act, outb, in_sem, w_sem, out_sem, mix_sem,
):
    me, side = lax.axis_index("dp"), lax.axis_index("fsdp")
    proj = weight_copies(side, o0, o1, w_out, w_sem.at[0])
    ups = weight_copies(side, u0, u1, w_up, w_sem.at[1])
    downs = weight_copies(side, d0, d1, w_down, w_sem.at[2])

    def mix_copy(m):
        part = pl.ds(m * 256, 256)
        return pltpu.make_async_copy(attended.at[part, :], normed.at[part, :], mix_sem.at[m])

    mix_copy(0).start()
    run(proj, "start")
    load_sequences(side, order, arrived, sent, xs, in_sem, 0, 8)
    run(ups + downs, "start")
    load_sequences(side, order, arrived, sent, xs, in_sem, 8, BLK)
    for m in range(1, 4):
        mix_copy(m).start()

    def block(m, first):
        base = m * 256 if first else pl.multiple_of(m * 256, 256)
        mix_copy(m).wait()
        if first:
            run(proj, "wait")
        for j in range(8):
            await_sequence(sent, xs, in_sem, m * 8 + j)
        columns = jnp.concatenate([marks_of(xs, m * 2 + g)[1] for g in range(2)], axis=0)
        part = jnp.dot(
            normed[pl.ds(base, 256), :], w_out[...], preferred_element_type=jnp.float32
        )
        for j in range(8):
            k = m * 8 + j
            total = sequence(xs, k).astype(jnp.float32) + part[j * SEQ:(j + 1) * SEQ, :]
            mid[j * SEQ:(j + 1) * SEQ, :] = total
            second[j * SEQ:(j + 1) * SEQ, :] = norm(total).astype(jnp.bfloat16)
        if first:
            run(ups, "wait")
        for n in range(MLP // UP):
            upper = jnp.dot(
                second[...], w_up[:, n * UP:(n + 1) * UP], preferred_element_type=jnp.float32
            )
            act[:, n * UP:(n + 1) * UP] = gelu(upper).astype(jnp.bfloat16)
        if first:
            run(downs, "wait")
        for n in range(D // DOWN):
            lower = jnp.dot(
                act[...], w_down[:, n * DOWN:(n + 1) * DOWN], preferred_element_type=jnp.float32
            )
            total = mid[:, n * DOWN:(n + 1) * DOWN] + lower
            total = jnp.where(columns > 0.0, total, 0.0).astype(jnp.bfloat16)
            for j in range(8):
                outb[m * 8 + j, :, n * DOWN:(n + 1) * DOWN] = total[j * SEQ:(j + 1) * SEQ, :]
        for j in range(8):
            k = m * 8 + j

            @pl.when(side == 0)
            def _():
                pltpu.make_async_copy(outb.at[k], out.at[k], out_sem.at[k]).start()

            @pl.when(side == 1)
            def _():
                pltpu.make_async_copy(
                    outb.at[k], results.at[table[0, k, me]], out_sem.at[k]
                ).start()

    block(0, True)
    lax.fori_loop(1, 4, lambda m, carry: (block(m, False), carry)[1], 0)
    for k in range(BLK):
        pltpu.make_async_copy(outb.at[k], out.at[k], out_sem.at[k]).wait()


def mlp_kernel(*operands):
    bf, f32 = jnp.bfloat16, jnp.float32
    return pl.pallas_call(
        mlp_body,
        out_shape=(
            jax.ShapeDtypeStruct((BLK, SEQ, D), bf),
            jax.ShapeDtypeStruct((PEERS, SEQ, D), bf),
        ),
        in_specs=[SMEM, SMEM, ANY] + [HBM] * 8,
        out_specs=(HBM, HBM),
        scratch_shapes=[
            pltpu.VMEM((BLK, SLOT, 128), bf),
            pltpu.VMEM((D, D), bf),
            pltpu.VMEM((D, MLP), bf),
            pltpu.VMEM((MLP, D), bf),
            pltpu.VMEM((ROWS, D), bf),
            pltpu.VMEM((256, D), bf),
            pltpu.VMEM((256, D), f32),
            pltpu.VMEM((256, MLP), bf),
            pltpu.VMEM((BLK, SEQ, D), bf),
            pltpu.SemaphoreType.DMA((BLK,)),
            pltpu.SemaphoreType.DMA((3, 2)),
            pltpu.SemaphoreType.DMA((BLK,)),
            pltpu.SemaphoreType.DMA((4,)),
        ],
        cost_estimate=pl.CostEstimate(
            flops=20_000_000_000, bytes_accessed=25_000_000, transcendentals=4_000_000
        ),
        compiler_params=pltpu.CompilerParams(vmem_limit_bytes=VMEM_LIMIT),
        name="mlp",
    )(*operands)


def settle_body(order, returned, out_in, out, buf, in_sem, out_sem):
    def in_copy(k):
        return pltpu.make_async_copy(returned.at[order[k, 0]], buf.at[k], in_sem.at[k])

    def out_copy(k):
        return pltpu.make_async_copy(buf.at[k], out.at[k], out_sem.at[k])

    @pl.when(lax.axis_index("fsdp") == 1)
    def _():
        for k in range(BLK):
            in_copy(k).start()
        for k in range(BLK):
            in_copy(k).wait()
            out_copy(k).start()
        for k in range(BLK):
            out_copy(k).wait()


def settle_kernel(order, returned, out):
    return pl.pallas_call(
        settle_body,
        out_shape=jax.ShapeDtypeStruct(out.shape, out.dtype),
        in_specs=[SMEM, HBM, HBM],
        out_specs=HBM,
        scratch_shapes=[
            pltpu.VMEM((BLK, SEQ, D), jnp.bfloat16),
            pltpu.SemaphoreType.DMA((BLK,)),
            pltpu.SemaphoreType.DMA((BLK,)),
        ],
        input_output_aliases={2: 0},
        compiler_params=pltpu.CompilerParams(vmem_limit_bytes=VMEM_LIMIT),
        name="settle",
    )(order, returned, out)


def blank(like):
    return pl.pallas_call(
        lambda ref, out: None,
        out_shape=jax.ShapeDtypeStruct(like.shape, like.dtype),
        in_specs=[HBM],
        out_specs=HBM,
        name="blank",
    )(like)


def exchange(chosen, values):
    return lax.cond(
        chosen,
        lambda x: lax.all_to_all(x, "dp", split_axis=0, concat_axis=0, tiled=True),
        blank,
        values,
    )


def local(
    patches, rows, cols, keep, images, destination, row_table, col_table, w_qkv, w_out, w_up, w_down
):
    side = lax.axis_index("fsdp")
    swap = [(0, 1), (1, 0)]
    pairs = []
    for w in (w_qkv, w_out, w_up, w_down):
        pairs.append((w, lax.ppermute(w, "fsdp", swap)))
    table = jnp.transpose(destination, (0, 2, 1))
    sent, order = embed_slots(
        table, table, rows, cols, keep, images, row_table, col_table, patches
    )
    arrived = exchange(side == 0, sent)
    attended = attend_kernel(order, arrived, sent, *pairs[0])
    out, results = mlp_kernel(
        order, table, attended, arrived, sent, *pairs[1], *pairs[2], *pairs[3]
    )
    returned = exchange(side == 1, results)
    return settle_kernel(order, returned, out)


def solution(mesh):
    whole = P(("dp", "fsdp"), None, None)
    flat = P(("dp", "fsdp"), None)
    half = P("fsdp", None)
    in_specs = (
        whole, flat, flat, flat, flat, P("fsdp", None, None), P(), P(), half, half, half, half,
    )
    return jax.shard_map(local, mesh=mesh, in_specs=in_specs, out_specs=whole, check_vma=False)
```

```python
import jax
import jax.numpy as jnp
from jax import lax
from jax.experimental import pallas as pl
from jax.experimental.pallas import tpu as pltpu
from jax.sharding import PartitionSpec as P


HEADS = 16
HEAD_DIM = 64
BLK = 32
SEQ = 32
D = 1024
MLP = 4096
PEERS = 64
GRID = 64
ROWS = BLK * SEQ
COLS = D // 128
SLOT = COLS * SEQ + 8
GROUP = 4
EPS = 1e-06
UP = 512
DOWN = 256
MASKED = -1e30
VMEM_LIMIT = 60 * 1024 * 1024
EMBED_LIMIT = 60 * 1024 * 1024
ATTEND_LIMIT = 24 * 1024 * 1024
MLP_LIMIT = 34 * 1024 * 1024
WIDE = 512
RB = 256
RS = RB // SEQ
QB = 512
QS = QB // SEQ
ANY = pl.BlockSpec(memory_space=pl.ANY)
HBM = pl.BlockSpec(memory_space=pltpu.HBM)
SMEM = pl.BlockSpec(memory_space=pltpu.SMEM)
VMEM = pl.BlockSpec(memory_space=pltpu.VMEM)


def norm(values):
    center = values - jnp.mean(values, axis=-1, keepdims=True)
    spread = jnp.mean(center * center, axis=-1, keepdims=True)
    return center * lax.rsqrt(spread + EPS)


def gelu(x):
    inner = x * (0.7978845608028654 + 0.035677408136300125 * (x * x))
    half = 0.5 * x
    return half + half * jnp.tanh(inner)


def embed_body(
    table, wide_in, rows_in, cols_in, keep_in, images_in, row_table, col_table, patches,
    out, order,
    buf, raw, tables, marks, spots, wide_table, rows, cols, keep, images, in_sem, small_sem, sem,
):
    me, side = lax.axis_index("dp"), lax.axis_index("fsdp")

    def in_copy(g):
        part = pl.ds(g * 2 * GROUP, 2 * GROUP)
        return pltpu.make_async_copy(patches.at[part], raw.at[part], in_sem.at[g])

    def out_copy(k):
        slot = jnp.where(side == 0, table[0, k, me], k)
        return pltpu.make_async_copy(buf.at[k], out.at[slot], sem.at[k])

    small = [
        (keep_in, keep), (images_in, images), (rows_in, rows), (cols_in, cols),
        (row_table, tables.at[:GRID, :]), (col_table, tables.at[GRID:, :]), (wide_in, wide_table),
    ]
    small = [
        pltpu.make_async_copy(source, target, small_sem.at[i])
        for i, (source, target) in enumerate(small)
    ]
    run(small, "start")
    for g in range(BLK // GROUP // 2):
        in_copy(g).start()
    run(small, "wait")
    label = (keep[...] * (images[...] + 1)).astype(jnp.float32)
    marks[...] = jnp.concatenate([label] * GROUP, axis=1)
    for i, ref in enumerate((rows, cols)):
        parts = [ref[pl.ds(j, BLK // GROUP, stride=GROUP), :] for j in range(GROUP)]
        spots[i] = jnp.concatenate(parts, axis=1)
    slots = lax.broadcasted_iota(jnp.int32, (2 * GRID, 128), 0)
    for g in range(BLK // GROUP):
        row, col = spots[0, g:g + 1, :], spots[1, g:g + 1, :] + GRID
        onehot = jnp.where((slots == row) | (slots == col), 1.0, 0.0).astype(jnp.bfloat16)
        places = lax.dot_general(
            onehot, tables[...], (((0,), (0,)), ((), ())), preferred_element_type=jnp.float32
        )
        if g % 2 == 0:
            in_copy(g // 2).wait()
        for j in range(GROUP):
            k = g * GROUP + j
            block = raw[k].astype(jnp.float32) + places[j * SEQ:(j + 1) * SEQ, :]
            block = block.astype(jnp.bfloat16)
            for c in range(COLS):
                buf[k, c * SEQ:(c + 1) * SEQ, :] = block[:, c * 128:(c + 1) * 128]
            mark = jnp.broadcast_to(marks[k:k + 1, :], (8, 128))
            buf[k, COLS * SEQ:, :] = mark.astype(jnp.bfloat16)
            out_copy(k).start()
    hits = jnp.where(wide_table[0] == me, 1.0, 0.0)
    filled = jnp.broadcast_to(jnp.max(hits, axis=0, keepdims=True), (BLK, PEERS))
    before = lax.broadcasted_iota(jnp.int32, (PEERS, PEERS), 0)
    after = lax.broadcasted_iota(jnp.int32, (PEERS, PEERS), 1)
    earlier = jnp.where(before < after, 1.0, 0.0).astype(jnp.bfloat16)
    rank = jnp.dot(filled.astype(jnp.bfloat16), earlier, preferred_element_type=jnp.float32)
    wanted = lax.broadcasted_iota(jnp.int32, (BLK, PEERS), 0).astype(jnp.float32)
    source = lax.broadcasted_iota(jnp.int32, (BLK, PEERS), 1).astype(jnp.float32)
    picked = jnp.where((filled > 0.0) & (rank == wanted), source, 0.0)
    picked = jnp.sum(picked, axis=1, keepdims=True)
    order[...] = jnp.broadcast_to(picked, (BLK, 128)).astype(jnp.int32)
    for k in range(BLK):
        out_copy(k).wait()


def embed_slots(*operands):
    return pl.pallas_call(
        embed_body,
        out_shape=(
            jax.ShapeDtypeStruct((PEERS, SLOT, 128), jnp.bfloat16),
            jax.ShapeDtypeStruct((BLK, 128), jnp.int32),
        ),
        in_specs=[SMEM] + [ANY] * 8,
        out_specs=(HBM, VMEM),
        scratch_shapes=[
            pltpu.VMEM((BLK, SLOT, 128), jnp.bfloat16),
            pltpu.VMEM((BLK, SEQ, D), jnp.bfloat16),
            pltpu.VMEM((2 * GRID, D), jnp.bfloat16),
            pltpu.VMEM((BLK, 128), jnp.float32),
            pltpu.VMEM((2, BLK // GROUP, 128), jnp.int32),
            pltpu.VMEM((1, BLK, PEERS), jnp.int32),
            pltpu.VMEM((BLK, SEQ), jnp.int32),
            pltpu.VMEM((BLK, SEQ), jnp.int32),
            pltpu.VMEM((BLK, SEQ), jnp.int32),
            pltpu.VMEM((BLK, SEQ), jnp.int32),
            pltpu.SemaphoreType.DMA((BLK // GROUP // 2,)),
            pltpu.SemaphoreType.DMA((7,)),
            pltpu.SemaphoreType.DMA((BLK,)),
        ],
        compiler_params=pltpu.CompilerParams(vmem_limit_bytes=EMBED_LIMIT),
        name="embed",
    )(*operands)


def sequence(xs, k):
    return jnp.concatenate([xs[k, c * SEQ:(c + 1) * SEQ, :] for c in range(COLS)], axis=1)


def weight_copies(side, own, other, whole, sem):
    half = own.shape[0]
    return [
        pltpu.make_async_copy(piece, whole.at[pl.ds(row * half, half), :], sem.at[i])
        for i, (piece, row) in enumerate(((own, side), (other, 1 - side)))
    ]


def run(copies, act):
    for copy in copies:
        getattr(copy, act)()


def marks_of(xs, g):
    lane = lax.broadcasted_iota(jnp.int32, (128, 128), 1)
    line = lax.broadcasted_iota(jnp.int32, (128, 128), 0)
    label = jnp.zeros((8, 128), jnp.float32)
    for j in range(GROUP):
        marks = xs[g * GROUP + j, COLS * SEQ:, :].astype(jnp.float32)
        label = jnp.where(lane[:8] // SEQ == j, marks, label)
    wide = jnp.broadcast_to(label[:1], (128, 128))
    column = jnp.sum(jnp.where(lane == line, wide, 0.0), axis=1, keepdims=True)
    return wide, column


def load_sequences(side, order, arrived, sent, xs, sem, low, high):
    for k in range(low, high):
        @pl.when(side == 0)
        def _():
            pltpu.make_async_copy(arrived.at[order[k, 0]], xs.at[k], sem.at[k]).start()

        @pl.when(side == 1)
        def _():
            pltpu.make_async_copy(sent.at[k], xs.at[k], sem.at[k]).start()


def await_sequence(sent, xs, sem, k):
    pltpu.make_async_copy(sent.at[k], xs.at[k], sem.at[k]).wait()


def attend_body(
    order, arrived, sent, own, other, out, kept,
    xs, w_qkv, normed, qkv, mixed, in_sem, w_sem, out_sem, keep_sem,
):
    side = lax.axis_index("fsdp")
    copies = weight_copies(side, own, other, w_qkv, w_sem.at[0])

    def out_copy(g):
        part = pl.ds(g * 128, 128)
        return pltpu.make_async_copy(mixed.at[part, :], out.at[part, :], out_sem.at[g])

    load_sequences(side, order, arrived, sent, xs, in_sem, 0, QS)
    run(copies, "start")
    load_sequences(side, order, arrived, sent, xs, in_sem, QS, BLK)

    def smooth(m, slot):
        for j in range(QS):
            x = sequence(xs, m * QS + j).astype(jnp.float32)
            normed[slot, j * SEQ:(j + 1) * SEQ, :] = norm(x).astype(jnp.bfloat16)

    def project(m, slot):
        base = m * QB if isinstance(m, int) else pl.multiple_of(m * QB, QB)
        for n in range(3 * D // WIDE):
            part = jnp.dot(
                normed[slot], w_qkv[:, n * WIDE:(n + 1) * WIDE],
                preferred_element_type=jnp.float32,
            )
            qkv[pl.ds(base, QB), n * WIDE:(n + 1) * WIDE] = part.astype(jnp.bfloat16)

    for j in range(QS):
        await_sequence(sent, xs, in_sem, j)
    smooth(0, 0)
    for j in range(QS, BLK):
        await_sequence(sent, xs, in_sem, j)
    keeping = pltpu.make_async_copy(xs, kept, keep_sem)
    keeping.start()
    run(copies, "wait")

    def block(m, carry):
        slot = m % 2
        project(m, slot)
        smooth(m + 1, 1 - slot)
        return carry

    lax.fori_loop(0, ROWS // QB - 1, block, 0)
    project(ROWS // QB - 1, 1)
    lane = lax.broadcasted_iota(jnp.int32, (128, 128), 1)
    line = lax.broadcasted_iota(jnp.int32, (128, 128), 0)
    low = lane < HEAD_DIM
    zero = jnp.zeros((128, 128), jnp.bfloat16)
    one = jnp.ones((128, 128), jnp.bfloat16)
    ones = jnp.concatenate([jnp.where(low, one, zero), jnp.where(low, zero, one)], axis=0)

    def attend(g, carry):
        base = pl.multiple_of(g * 128, 128)
        wide, column = marks_of(xs, g)
        allowed = (column == wide) & (wide > 0.0) & (lane // SEQ == line // SEQ)
        bias = jnp.where(allowed, 0.0, MASKED)
        bias = jnp.concatenate([bias, bias], axis=0)
        dropped = jnp.where(column == 0.0, 1.0, 0.0)
        for h in range(HEADS // 2):
            q = qkv[pl.ds(base, 128), h * 128:(h + 1) * 128] * jnp.bfloat16(HEAD_DIM ** -0.5)
            key = qkv[pl.ds(base, 128), D + h * 128:D + (h + 1) * 128]
            value = qkv[pl.ds(base, 128), 2 * D + h * 128:2 * D + (h + 1) * 128]
            both = jnp.concatenate([jnp.where(low, q, zero), jnp.where(low, zero, q)], axis=0)
            scores = lax.dot_general(
                both, key, (((1,), (1,)), ((), ())), preferred_element_type=jnp.float32
            )
            scores = scores + bias
            peak = jnp.maximum(jnp.max(scores, axis=1, keepdims=True), 0.1 * MASKED)
            weights = jnp.exp(scores - peak).astype(jnp.bfloat16)
            weights = jnp.concatenate([weights[:128], weights[128:]], axis=1)
            stacked = jnp.concatenate(
                [jnp.where(low, value, zero), jnp.where(low, zero, value)], axis=0
            )
            stacked = jnp.concatenate([stacked, ones], axis=1)
            both = jnp.dot(weights, stacked, preferred_element_type=jnp.float32)
            result = both[:, :128] / (both[:, 128:] + dropped)
            mixed[pl.ds(base, 128), h * 128:(h + 1) * 128] = result.astype(jnp.bfloat16)
        out_copy(g).start()
        return carry

    lax.fori_loop(0, BLK // GROUP, attend, 0)
    for g in range(BLK // GROUP):
        out_copy(g).wait()
    keeping.wait()


def attend_kernel(order, arrived, sent, own, other):
    bf = jnp.bfloat16
    return pl.pallas_call(
        attend_body,
        out_shape=(
            jax.ShapeDtypeStruct((ROWS, D), bf),
            jax.ShapeDtypeStruct((BLK, SLOT, 128), bf),
        ),
        in_specs=[SMEM, HBM, HBM, ANY, ANY],
        out_specs=(ANY, ANY),
        scratch_shapes=[
            pltpu.VMEM((BLK, SLOT, 128), bf),
            pltpu.VMEM((D, 3 * D), bf),
            pltpu.VMEM((2, QB, D), bf),
            pltpu.VMEM((ROWS, 3 * D), bf),
            pltpu.VMEM((ROWS, D), bf),
            pltpu.SemaphoreType.DMA((BLK,)),
            pltpu.SemaphoreType.DMA((1, 2)),
            pltpu.SemaphoreType.DMA((BLK // GROUP,)),
            pltpu.SemaphoreType.DMA,
        ],
        cost_estimate=pl.CostEstimate(
            flops=7_000_000_000, bytes_accessed=12_000_000, transcendentals=2_000_000
        ),
        compiler_params=pltpu.CompilerParams(vmem_limit_bytes=ATTEND_LIMIT),
        name="attend",
    )(order, arrived, sent, own, other)


def mlp_body(
    table, attended, kept, o0, o1, u0, u1, d0, d1, out, results,
    xs, w_out, w_up, w_down, normed, second, mid, act, outb, in_sem, w_sem, out_sem, mix_sem,
):
    me, side = lax.axis_index("dp"), lax.axis_index("fsdp")
    proj = weight_copies(side, o0, o1, w_out, w_sem.at[0])
    ups = weight_copies(side, u0, u1, w_up, w_sem.at[1])
    downs = weight_copies(side, d0, d1, w_down, w_sem.at[2])

    def mix_copy(m):
        part = pl.ds(m * RB, RB)
        return pltpu.make_async_copy(attended.at[part, :], normed.at[part, :], mix_sem.at[m])

    def part_copy(m):
        part = pl.ds(m * RS, RS)
        return pltpu.make_async_copy(kept.at[part], xs.at[part], in_sem.at[m])

    mix_copy(0).start()
    run(proj, "start")
    part_copy(0).start()
    run(ups + downs, "start")
    for m in range(1, ROWS // RB):
        part_copy(m).start()
        mix_copy(m).start()

    def block(m, first):
        base = m * RB if first else pl.multiple_of(m * RB, RB)
        mix_copy(m).wait()
        if first:
            run(proj, "wait")
        part_copy(m).wait()
        columns = jnp.concatenate([marks_of(xs, m * (RB // 128) + g)[1] for g in range(RB // 128)], axis=0)
        part = jnp.dot(
            normed[pl.ds(base, RB), :], w_out[...], preferred_element_type=jnp.float32
        )
        for j in range(RS):
            k = m * RS + j
            total = sequence(xs, k).astype(jnp.float32) + part[j * SEQ:(j + 1) * SEQ, :]
            mid[j * SEQ:(j + 1) * SEQ, :] = total
            second[j * SEQ:(j + 1) * SEQ, :] = norm(total).astype(jnp.bfloat16)
        if first:
            run(ups, "wait")
        for n in range(MLP // UP):
            upper = jnp.dot(
                second[...], w_up[:, n * UP:(n + 1) * UP], preferred_element_type=jnp.float32
            )
            act[:, n * UP:(n + 1) * UP] = gelu(upper).astype(jnp.bfloat16)
        if first:
            run(downs, "wait")
        for n in range(D // DOWN):
            lower = jnp.dot(
                act[...], w_down[:, n * DOWN:(n + 1) * DOWN], preferred_element_type=jnp.float32
            )
            total = mid[:, n * DOWN:(n + 1) * DOWN] + lower
            total = jnp.where(columns > 0.0, total, 0.0).astype(jnp.bfloat16)
            for j in range(RS):
                outb[m * RS + j, :, n * DOWN:(n + 1) * DOWN] = total[j * SEQ:(j + 1) * SEQ, :]
        for j in range(RS):
            k = m * RS + j

            @pl.when(side == 0)
            def _():
                pltpu.make_async_copy(outb.at[k], out.at[k], out_sem.at[k]).start()

            @pl.when(side == 1)
            def _():
                pltpu.make_async_copy(
                    outb.at[k], results.at[table[0, k, me]], out_sem.at[k]
                ).start()

    block(0, True)
    lax.fori_loop(1, ROWS // RB, lambda m, carry: (block(m, False), carry)[1], 0)
    for k in range(BLK):
        pltpu.make_async_copy(outb.at[k], out.at[k], out_sem.at[k]).wait()


def mlp_kernel(*operands):
    bf, f32 = jnp.bfloat16, jnp.float32
    return pl.pallas_call(
        mlp_body,
        out_shape=(
            jax.ShapeDtypeStruct((BLK, SEQ, D), bf),
            jax.ShapeDtypeStruct((PEERS, SEQ, D), bf),
        ),
        in_specs=[SMEM] + [ANY] * 8,
        out_specs=(HBM, HBM),
        scratch_shapes=[
            pltpu.VMEM((BLK, SLOT, 128), bf),
            pltpu.VMEM((D, D), bf),
            pltpu.VMEM((D, MLP), bf),
            pltpu.VMEM((MLP, D), bf),
            pltpu.VMEM((ROWS, D), bf),
            pltpu.VMEM((RB, D), bf),
            pltpu.VMEM((RB, D), f32),
            pltpu.VMEM((RB, MLP), bf),
            pltpu.VMEM((BLK, SEQ, D), bf),
            pltpu.SemaphoreType.DMA((ROWS // RB,)),
            pltpu.SemaphoreType.DMA((3, 2)),
            pltpu.SemaphoreType.DMA((BLK,)),
            pltpu.SemaphoreType.DMA((ROWS // RB,)),
        ],
        cost_estimate=pl.CostEstimate(
            flops=20_000_000_000, bytes_accessed=25_000_000, transcendentals=4_000_000
        ),
        compiler_params=pltpu.CompilerParams(vmem_limit_bytes=MLP_LIMIT),
        name="mlp",
    )(*operands)


def settle_body(order, returned, out_in, out, buf, in_sem, out_sem):
    def in_copy(k):
        return pltpu.make_async_copy(returned.at[order[k, 0]], buf.at[k], in_sem.at[k])

    def out_copy(k):
        return pltpu.make_async_copy(buf.at[k], out.at[k], out_sem.at[k])

    @pl.when(lax.axis_index("fsdp") == 1)
    def _():
        for k in range(BLK):
            in_copy(k).start()
        for k in range(BLK):
            in_copy(k).wait()
            out_copy(k).start()
        for k in range(BLK):
            out_copy(k).wait()


def settle_kernel(order, returned, out):
    return pl.pallas_call(
        settle_body,
        out_shape=jax.ShapeDtypeStruct(out.shape, out.dtype),
        in_specs=[SMEM, HBM, HBM],
        out_specs=HBM,
        scratch_shapes=[
            pltpu.VMEM((BLK, SEQ, D), jnp.bfloat16),
            pltpu.SemaphoreType.DMA((BLK,)),
            pltpu.SemaphoreType.DMA((BLK,)),
        ],
        input_output_aliases={2: 0},
        compiler_params=pltpu.CompilerParams(vmem_limit_bytes=VMEM_LIMIT),
        name="settle",
    )(order, returned, out)


def blank(like):
    return pl.pallas_call(
        lambda ref, out: None,
        out_shape=jax.ShapeDtypeStruct(like.shape, like.dtype),
        in_specs=[HBM],
        out_specs=HBM,
        name="blank",
    )(like)


def exchange(chosen, values):
    return lax.cond(
        chosen,
        lambda x: lax.all_to_all(x, "dp", split_axis=0, concat_axis=0, tiled=True),
        blank,
        values,
    )


def local(
    patches, rows, cols, keep, images, destination, row_table, col_table, w_qkv, w_out, w_up, w_down
):
    side = lax.axis_index("fsdp")
    swap = [(0, 1), (1, 0)]
    pairs = []
    for w in (w_qkv, w_out, w_up, w_down):
        pairs.append((w, lax.ppermute(w, "fsdp", swap)))
    table = jnp.transpose(destination, (0, 2, 1))
    sent, order = embed_slots(
        table, table, rows, cols, keep, images, row_table, col_table, patches
    )
    arrived = exchange(side == 0, sent)
    attended, kept = attend_kernel(order, arrived, sent, *pairs[0])
    out, results = mlp_kernel(table, attended, kept, *pairs[1], *pairs[2], *pairs[3])
    returned = exchange(side == 1, results)
    return settle_kernel(order, returned, out)


def solution(mesh):
    whole = P(("dp", "fsdp"), None, None)
    flat = P(("dp", "fsdp"), None)
    half = P("fsdp", None)
    in_specs = (
        whole, flat, flat, flat, flat, P("fsdp", None, None), P(), P(), half, half, half, half,
    )
    return jax.shard_map(local, mesh=mesh, in_specs=in_specs, out_specs=whole, check_vma=False)
```

```python
import jax
import jax.numpy as jnp
from jax import lax
from jax.experimental import pallas as pl
from jax.experimental.pallas import tpu as pltpu
from jax.sharding import PartitionSpec as P


HEADS = 16
HEAD_DIM = 64
BLK = 32
SEQ = 32
D = 1024
MLP = 4096
PEERS = 64
GRID = 64
ROWS = BLK * SEQ
COLS = D // 128
SLOT = COLS * SEQ + 8
GROUP = 4
EPS = 1e-06
UP = 512
DOWN = 256
MASKED = -1e30
VMEM_LIMIT = 60 * 1024 * 1024
EMBED_LIMIT = 60 * 1024 * 1024
ATTEND_LIMIT = 42 * 1024 * 1024
MLP_LIMIT = 36 * 1024 * 1024
WIDE = 512
BOTH = 2
RB = 256
RS = RB // SEQ
QB = 512
QS = QB // SEQ
ANY = pl.BlockSpec(memory_space=pl.ANY)
HBM = pl.BlockSpec(memory_space=pltpu.HBM)
SMEM = pl.BlockSpec(memory_space=pltpu.SMEM)
VMEM = pl.BlockSpec(memory_space=pltpu.VMEM)


def norm(values):
    center = values - jnp.mean(values, axis=-1, keepdims=True)
    spread = jnp.mean(center * center, axis=-1, keepdims=True)
    return center * lax.rsqrt(spread + EPS)


def gelu(x):
    inner = x * (0.7978845608028654 + 0.035677408136300125 * (x * x))
    half = 0.5 * x
    return half + half * jnp.tanh(inner)


def embed_body(
    table, wide_in, rows_in, cols_in, keep_in, images_in, row_table, col_table, patches,
    out, order,
    buf, raw, tables, marks, spots, wide_table, rows, cols, keep, images, in_sem, small_sem, sem,
):
    me, side = lax.axis_index("dp"), lax.axis_index("fsdp")

    def in_copy(g):
        part = pl.ds(g * 2 * GROUP, 2 * GROUP)
        return pltpu.make_async_copy(patches.at[part], raw.at[part], in_sem.at[g])

    def out_copy(k):
        slot = jnp.where(side == 0, table[0, k, me], k)
        return pltpu.make_async_copy(buf.at[k], out.at[slot], sem.at[k])

    small = [
        (keep_in, keep), (images_in, images), (rows_in, rows), (cols_in, cols),
        (row_table, tables.at[:GRID, :]), (col_table, tables.at[GRID:, :]), (wide_in, wide_table),
    ]
    small = [
        pltpu.make_async_copy(source, target, small_sem.at[i])
        for i, (source, target) in enumerate(small)
    ]
    run(small, "start")
    for g in range(BLK // GROUP // 2):
        in_copy(g).start()
    run(small, "wait")
    label = (keep[...] * (images[...] + 1)).astype(jnp.float32)
    marks[...] = jnp.concatenate([label] * GROUP, axis=1)
    for i, ref in enumerate((rows, cols)):
        parts = [ref[pl.ds(j, BLK // GROUP, stride=GROUP), :] for j in range(GROUP)]
        spots[i] = jnp.concatenate(parts, axis=1)
    slots = lax.broadcasted_iota(jnp.int32, (2 * GRID, 128), 0)
    for g in range(BLK // GROUP):
        row, col = spots[0, g:g + 1, :], spots[1, g:g + 1, :] + GRID
        onehot = jnp.where((slots == row) | (slots == col), 1.0, 0.0).astype(jnp.bfloat16)
        places = lax.dot_general(
            onehot, tables[...], (((0,), (0,)), ((), ())), preferred_element_type=jnp.float32
        )
        if g % 2 == 0:
            in_copy(g // 2).wait()
        for j in range(GROUP):
            k = g * GROUP + j
            block = raw[k].astype(jnp.float32) + places[j * SEQ:(j + 1) * SEQ, :]
            block = block.astype(jnp.bfloat16)
            for c in range(COLS):
                buf[k, c * SEQ:(c + 1) * SEQ, :] = block[:, c * 128:(c + 1) * 128]
            mark = jnp.broadcast_to(marks[k:k + 1, :], (8, 128))
            buf[k, COLS * SEQ:, :] = mark.astype(jnp.bfloat16)
            out_copy(k).start()
    hits = jnp.where(wide_table[0] == me, 1.0, 0.0)
    filled = jnp.broadcast_to(jnp.max(hits, axis=0, keepdims=True), (BLK, PEERS))
    before = lax.broadcasted_iota(jnp.int32, (PEERS, PEERS), 0)
    after = lax.broadcasted_iota(jnp.int32, (PEERS, PEERS), 1)
    earlier = jnp.where(before < after, 1.0, 0.0).astype(jnp.bfloat16)
    rank = jnp.dot(filled.astype(jnp.bfloat16), earlier, preferred_element_type=jnp.float32)
    wanted = lax.broadcasted_iota(jnp.int32, (BLK, PEERS), 0).astype(jnp.float32)
    source = lax.broadcasted_iota(jnp.int32, (BLK, PEERS), 1).astype(jnp.float32)
    picked = jnp.where((filled > 0.0) & (rank == wanted), source, 0.0)
    picked = jnp.sum(picked, axis=1, keepdims=True)
    order[...] = jnp.broadcast_to(picked, (BLK, 128)).astype(jnp.int32)
    for k in range(BLK):
        out_copy(k).wait()


def embed_slots(*operands):
    return pl.pallas_call(
        embed_body,
        out_shape=(
            jax.ShapeDtypeStruct((PEERS, SLOT, 128), jnp.bfloat16),
            jax.ShapeDtypeStruct((BLK, 128), jnp.int32),
        ),
        in_specs=[SMEM] + [ANY] * 8,
        out_specs=(HBM, VMEM),
        scratch_shapes=[
            pltpu.VMEM((BLK, SLOT, 128), jnp.bfloat16),
            pltpu.VMEM((BLK, SEQ, D), jnp.bfloat16),
            pltpu.VMEM((2 * GRID, D), jnp.bfloat16),
            pltpu.VMEM((BLK, 128), jnp.float32),
            pltpu.VMEM((2, BLK // GROUP, 128), jnp.int32),
            pltpu.VMEM((1, BLK, PEERS), jnp.int32),
            pltpu.VMEM((BLK, SEQ), jnp.int32),
            pltpu.VMEM((BLK, SEQ), jnp.int32),
            pltpu.VMEM((BLK, SEQ), jnp.int32),
            pltpu.VMEM((BLK, SEQ), jnp.int32),
            pltpu.SemaphoreType.DMA((BLK // GROUP // 2,)),
            pltpu.SemaphoreType.DMA((7,)),
            pltpu.SemaphoreType.DMA((BLK,)),
        ],
        compiler_params=pltpu.CompilerParams(vmem_limit_bytes=EMBED_LIMIT),
        name="embed",
    )(*operands)


def sequence(xs, k):
    return jnp.concatenate([xs[k, c * SEQ:(c + 1) * SEQ, :] for c in range(COLS)], axis=1)


def weight_copies(side, own, other, whole, sem):
    half = own.shape[0]
    return [
        pltpu.make_async_copy(piece, whole.at[pl.ds(row * half, half), :], sem.at[i])
        for i, (piece, row) in enumerate(((own, side), (other, 1 - side)))
    ]


def run(copies, act):
    for copy in copies:
        getattr(copy, act)()


def marks_of(xs, g):
    lane = lax.broadcasted_iota(jnp.int32, (128, 128), 1)
    line = lax.broadcasted_iota(jnp.int32, (128, 128), 0)
    label = jnp.zeros((8, 128), jnp.float32)
    for j in range(GROUP):
        marks = xs[g * GROUP + j, COLS * SEQ:, :].astype(jnp.float32)
        label = jnp.where(lane[:8] // SEQ == j, marks, label)
    wide = jnp.broadcast_to(label[:1], (128, 128))
    column = jnp.sum(jnp.where(lane == line, wide, 0.0), axis=1, keepdims=True)
    return wide, column


def load_sequences(side, order, arrived, sent, xs, sem, low, high):
    for k in range(low, high):
        @pl.when(side == 0)
        def _():
            pltpu.make_async_copy(arrived.at[order[k, 0]], xs.at[k], sem.at[k]).start()

        @pl.when(side == 1)
        def _():
            pltpu.make_async_copy(sent.at[k], xs.at[k], sem.at[k]).start()


def await_sequence(sent, xs, sem, k):
    pltpu.make_async_copy(sent.at[k], xs.at[k], sem.at[k]).wait()


def attend_body(
    order, arrived, sent, own, other, out, kept,
    xs, w_qkv, normed, qkv, mixed, in_sem, w_sem, out_sem, keep_sem,
):
    side = lax.axis_index("fsdp")
    copies = weight_copies(side, own, other, w_qkv, w_sem.at[0])

    def out_copy(g):
        part = pl.ds(g * 128, 128)
        return pltpu.make_async_copy(mixed.at[part, :], out.at[part, :], out_sem.at[g])

    load_sequences(side, order, arrived, sent, xs, in_sem, 0, QS)
    run(copies, "start")
    load_sequences(side, order, arrived, sent, xs, in_sem, QS, BLK)

    def smooth(m, slot):
        for j in range(QS):
            x = sequence(xs, m * QS + j).astype(jnp.float32)
            normed[slot, j * SEQ:(j + 1) * SEQ, :] = norm(x).astype(jnp.bfloat16)

    def project(m, slot):
        base = m * QB if isinstance(m, int) else pl.multiple_of(m * QB, QB)
        for n in range(3 * D // WIDE):
            part = jnp.dot(
                normed[slot], w_qkv[:, n * WIDE:(n + 1) * WIDE],
                preferred_element_type=jnp.float32,
            )
            qkv[pl.ds(base, QB), n * WIDE:(n + 1) * WIDE] = part.astype(jnp.bfloat16)

    for j in range(QS):
        await_sequence(sent, xs, in_sem, j)
    smooth(0, 0)
    for j in range(QS, BLK):
        await_sequence(sent, xs, in_sem, j)
    keeping = pltpu.make_async_copy(xs, kept, keep_sem)
    keeping.start()
    run(copies, "wait")

    def block(m, carry):
        slot = m % 2
        project(m, slot)
        smooth(m + 1, 1 - slot)
        return carry

    lax.fori_loop(0, ROWS // QB - 1, block, 0)
    project(ROWS // QB - 1, 1)
    lane = lax.broadcasted_iota(jnp.int32, (128, 128), 1)
    line = lax.broadcasted_iota(jnp.int32, (128, 128), 0)
    low = lane < HEAD_DIM
    zero = jnp.zeros((128, 128), jnp.bfloat16)
    one = jnp.ones((128, 128), jnp.bfloat16)
    ones = jnp.concatenate([jnp.where(low, one, zero), jnp.where(low, zero, one)], axis=0)

    def attend(g):
        base = pl.multiple_of(g * 128, 128)
        wide, column = marks_of(xs, g)
        allowed = (column == wide) & (wide > 0.0) & (lane // SEQ == line // SEQ)
        bias = jnp.where(allowed, 0.0, MASKED)
        bias = jnp.concatenate([bias, bias], axis=0)
        dropped = jnp.where(column == 0.0, 1.0, 0.0)
        for h in range(HEADS // 2):
            q = qkv[pl.ds(base, 128), h * 128:(h + 1) * 128] * jnp.bfloat16(HEAD_DIM ** -0.5)
            key = qkv[pl.ds(base, 128), D + h * 128:D + (h + 1) * 128]
            value = qkv[pl.ds(base, 128), 2 * D + h * 128:2 * D + (h + 1) * 128]
            both = jnp.concatenate([jnp.where(low, q, zero), jnp.where(low, zero, q)], axis=0)
            scores = lax.dot_general(
                both, key, (((1,), (1,)), ((), ())), preferred_element_type=jnp.float32
            )
            scores = scores + bias
            peak = jnp.maximum(jnp.max(scores, axis=1, keepdims=True), 0.1 * MASKED)
            weights = jnp.exp(scores - peak).astype(jnp.bfloat16)
            weights = jnp.concatenate([weights[:128], weights[128:]], axis=1)
            stacked = jnp.concatenate(
                [jnp.where(low, value, zero), jnp.where(low, zero, value)], axis=0
            )
            stacked = jnp.concatenate([stacked, ones], axis=1)
            both = jnp.dot(weights, stacked, preferred_element_type=jnp.float32)
            result = both[:, :128] / (both[:, 128:] + dropped)
            mixed[pl.ds(base, 128), h * 128:(h + 1) * 128] = result.astype(jnp.bfloat16)
        out_copy(g).start()

    def several(i, carry):
        for g in range(BOTH):
            attend(i * BOTH + g)
        return carry

    lax.fori_loop(0, BLK // GROUP // BOTH, several, 0)
    for g in range(BLK // GROUP):
        out_copy(g).wait()
    keeping.wait()


def attend_kernel(order, arrived, sent, own, other):
    bf = jnp.bfloat16
    return pl.pallas_call(
        attend_body,
        out_shape=(
            jax.ShapeDtypeStruct((ROWS, D), bf),
            jax.ShapeDtypeStruct((BLK, SLOT, 128), bf),
        ),
        in_specs=[SMEM, HBM, HBM, ANY, ANY],
        out_specs=(ANY, ANY),
        scratch_shapes=[
            pltpu.VMEM((BLK, SLOT, 128), bf),
            pltpu.VMEM((D, 3 * D), bf),
            pltpu.VMEM((2, QB, D), bf),
            pltpu.VMEM((ROWS, 3 * D), bf),
            pltpu.VMEM((ROWS, D), bf),
            pltpu.SemaphoreType.DMA((BLK,)),
            pltpu.SemaphoreType.DMA((1, 2)),
            pltpu.SemaphoreType.DMA((BLK // GROUP,)),
            pltpu.SemaphoreType.DMA,
        ],
        cost_estimate=pl.CostEstimate(
            flops=7_000_000_000, bytes_accessed=12_000_000, transcendentals=2_000_000
        ),
        compiler_params=pltpu.CompilerParams(vmem_limit_bytes=ATTEND_LIMIT),
        name="attend",
    )(order, arrived, sent, own, other)


def mlp_body(
    table, attended, kept, o0, o1, u0, u1, d0, d1, out, results,
    xs, w_out, w_up, w_down, normed, second, mid, act, outb, in_sem, w_sem, out_sem, mix_sem,
):
    me, side = lax.axis_index("dp"), lax.axis_index("fsdp")
    proj = weight_copies(side, o0, o1, w_out, w_sem.at[0])
    ups = weight_copies(side, u0, u1, w_up, w_sem.at[1])
    downs = weight_copies(side, d0, d1, w_down, w_sem.at[2])

    def mix_copy(m):
        part = pl.ds(m * RB, RB)
        return pltpu.make_async_copy(attended.at[part, :], normed.at[part, :], mix_sem.at[m])

    def part_copy(m):
        part = pl.ds(m * RS, RS)
        return pltpu.make_async_copy(kept.at[part], xs.at[part], in_sem.at[m])

    mix_copy(0).start()
    run(proj, "start")
    part_copy(0).start()
    run(ups + downs, "start")
    for m in range(1, ROWS // RB):
        part_copy(m).start()
        mix_copy(m).start()

    def front(m, slot):
        base = m * RB if isinstance(m, int) else pl.multiple_of(m * RB, RB)
        part = jnp.dot(
            normed[pl.ds(base, RB), :], w_out[...], preferred_element_type=jnp.float32
        )
        for j in range(RS):
            total = sequence(xs, m * RS + j).astype(jnp.float32) + part[j * SEQ:(j + 1) * SEQ, :]
            mid[slot, j * SEQ:(j + 1) * SEQ, :] = total
            second[slot, j * SEQ:(j + 1) * SEQ, :] = norm(total).astype(jnp.bfloat16)

    def block(m, first, last):
        slot = m % 2
        if first:
            mix_copy(0).wait()
            part_copy(0).wait()
            run(proj, "wait")
            front(0, 0)
        if not last:
            mix_copy(m + 1).wait()
            part_copy(m + 1).wait()
        columns = jnp.concatenate(
            [marks_of(xs, m * (RB // 128) + g)[1] for g in range(RB // 128)], axis=0
        )
        if first:
            run(ups, "wait")
        for n in range(MLP // UP):
            upper = jnp.dot(
                second[slot], w_up[:, n * UP:(n + 1) * UP], preferred_element_type=jnp.float32
            )
            act[:, n * UP:(n + 1) * UP] = gelu(upper).astype(jnp.bfloat16)
        if not last:
            front(m + 1, 1 - slot)
        if first:
            run(downs, "wait")
        for n in range(D // DOWN):
            lower = jnp.dot(
                act[...], w_down[:, n * DOWN:(n + 1) * DOWN], preferred_element_type=jnp.float32
            )
            total = mid[slot, :, n * DOWN:(n + 1) * DOWN] + lower
            total = jnp.where(columns > 0.0, total, 0.0).astype(jnp.bfloat16)
            for j in range(RS):
                outb[m * RS + j, :, n * DOWN:(n + 1) * DOWN] = total[j * SEQ:(j + 1) * SEQ, :]
        for j in range(RS):
            k = m * RS + j

            @pl.when(side == 0)
            def _():
                pltpu.make_async_copy(outb.at[k], out.at[k], out_sem.at[k]).start()

            @pl.when(side == 1)
            def _():
                pltpu.make_async_copy(
                    outb.at[k], results.at[table[0, k, me]], out_sem.at[k]
                ).start()

    final = ROWS // RB - 1
    block(0, True, False)
    lax.fori_loop(1, final, lambda m, carry: (block(m, False, False), carry)[1], 0)
    block(final, False, True)
    for k in range(BLK):
        pltpu.make_async_copy(outb.at[k], out.at[k], out_sem.at[k]).wait()


def mlp_kernel(*operands):
    bf, f32 = jnp.bfloat16, jnp.float32
    return pl.pallas_call(
        mlp_body,
        out_shape=(
            jax.ShapeDtypeStruct((BLK, SEQ, D), bf),
            jax.ShapeDtypeStruct((PEERS, SEQ, D), bf),
        ),
        in_specs=[SMEM] + [ANY] * 8,
        out_specs=(HBM, HBM),
        scratch_shapes=[
            pltpu.VMEM((BLK, SLOT, 128), bf),
            pltpu.VMEM((D, D), bf),
            pltpu.VMEM((D, MLP), bf),
            pltpu.VMEM((MLP, D), bf),
            pltpu.VMEM((ROWS, D), bf),
            pltpu.VMEM((2, RB, D), bf),
            pltpu.VMEM((2, RB, D), f32),
            pltpu.VMEM((RB, MLP), bf),
            pltpu.VMEM((BLK, SEQ, D), bf),
            pltpu.SemaphoreType.DMA((ROWS // RB,)),
            pltpu.SemaphoreType.DMA((3, 2)),
            pltpu.SemaphoreType.DMA((BLK,)),
            pltpu.SemaphoreType.DMA((ROWS // RB,)),
        ],
        cost_estimate=pl.CostEstimate(
            flops=20_000_000_000, bytes_accessed=25_000_000, transcendentals=4_000_000
        ),
        compiler_params=pltpu.CompilerParams(vmem_limit_bytes=MLP_LIMIT),
        name="mlp",
    )(*operands)


def settle_body(order, returned, out_in, out, buf, in_sem, out_sem):
    def in_copy(k):
        return pltpu.make_async_copy(returned.at[order[k, 0]], buf.at[k], in_sem.at[k])

    def out_copy(k):
        return pltpu.make_async_copy(buf.at[k], out.at[k], out_sem.at[k])

    @pl.when(lax.axis_index("fsdp") == 1)
    def _():
        for k in range(BLK):
            in_copy(k).start()
        for k in range(BLK):
            in_copy(k).wait()
            out_copy(k).start()
        for k in range(BLK):
            out_copy(k).wait()


def settle_kernel(order, returned, out):
    return pl.pallas_call(
        settle_body,
        out_shape=jax.ShapeDtypeStruct(out.shape, out.dtype),
        in_specs=[SMEM, HBM, HBM],
        out_specs=HBM,
        scratch_shapes=[
            pltpu.VMEM((BLK, SEQ, D), jnp.bfloat16),
            pltpu.SemaphoreType.DMA((BLK,)),
            pltpu.SemaphoreType.DMA((BLK,)),
        ],
        input_output_aliases={2: 0},
        compiler_params=pltpu.CompilerParams(vmem_limit_bytes=VMEM_LIMIT),
        name="settle",
    )(order, returned, out)


def blank(like):
    return pl.pallas_call(
        lambda ref, out: None,
        out_shape=jax.ShapeDtypeStruct(like.shape, like.dtype),
        in_specs=[HBM],
        out_specs=HBM,
        name="blank",
    )(like)


def exchange(chosen, values):
    return lax.cond(
        chosen,
        lambda x: lax.all_to_all(x, "dp", split_axis=0, concat_axis=0, tiled=True),
        blank,
        values,
    )


def local(
    patches, rows, cols, keep, images, destination, row_table, col_table, w_qkv, w_out, w_up, w_down
):
    side = lax.axis_index("fsdp")
    swap = [(0, 1), (1, 0)]
    pairs = []
    for w in (w_qkv, w_out, w_up, w_down):
        pairs.append((w, lax.ppermute(w, "fsdp", swap)))
    table = jnp.transpose(destination, (0, 2, 1))
    sent, order = embed_slots(
        table, table, rows, cols, keep, images, row_table, col_table, patches
    )
    arrived = exchange(side == 0, sent)
    attended, kept = attend_kernel(order, arrived, sent, *pairs[0])
    out, results = mlp_kernel(table, attended, kept, *pairs[1], *pairs[2], *pairs[3])
    returned = exchange(side == 1, results)
    return settle_kernel(order, returned, out)


def solution(mesh):
    whole = P(("dp", "fsdp"), None, None)
    flat = P(("dp", "fsdp"), None)
    half = P("fsdp", None)
    in_specs = (
        whole, flat, flat, flat, flat, P("fsdp", None, None), P(), P(), half, half, half, half,
    )
    return jax.shard_map(local, mesh=mesh, in_specs=in_specs, out_specs=whole, check_vma=False)
```
